32 devices in a mesh: gx: 4 (over y, core), gy: 2 (over x), gz: 4 (over z).
Axes of the slice: x: 2, y: 2, z: 4, core: 2. Of those that a mesh axis runs over, the one named last changes fastest.
Arguments:
- noisy_image: float32 [32, 64, 512], P('gz', 'gy', 'gx'), may hold values from -6 to 6
- fidelity: float32 [32, 64, 512], P('gz', 'gy', 'gx'), may hold values from 0.5 to 8
- primal_u: float32 [32, 64, 512], P('gz', 'gy', 'gx'), may hold values from -6 to 6
- primal_v: float32 [3, 32, 64, 512], P(None, 'gz', 'gy', 'gx'), may hold values from -2 to 2
- dual_p: float32 [3, 32, 64, 512], P(None, 'gz', 'gy', 'gx'), may hold values from -2.5 to 2.5
- dual_q: float32 [6, 32, 64, 512], P(None, 'gz', 'gy', 'gx'), may hold values from -2.5 to 2.5
Outputs:
- denoised: float32 [32, 64, 512], P('gz', 'gy', 'gx')
- vector_field: float32 [3, 32, 64, 512], P(None, 'gz', 'gy', 'gx')
- grad_dual: float32 [3, 32, 64, 512], P(None, 'gz', 'gy', 'gx')
- sym_dual: float32 [6, 32, 64, 512], P(None, 'gz', 'gy', 'gx')
The draws below stay inside these ranges and needn't reach their ends.
All inputs are finite; a program needn't handle non-finite values.
Results may differ from the reference program's by a relative error of at most 0.0001.
Values sent between devices are 32-bit elements; how exact they have to be, the bound alone decides.
No kernel may reach another device: no remote copies, remote signals or barrier semaphores. Data moves between devices by JAX's collectives and lax.ppermute only.
A program may use at most 64 MiB of HBM per device.

```python
import math
import jax
import jax.numpy as jnp
from jax import lax

ITERS = 3
NX = 512
NY = 64
NZ = 32


def shard_levels(stream_key, shape, split, smallest, largest):
    def one(dim, shards_of):
        draws = jax.random.uniform(jax.random.fold_in(jax.random.fold_in(stream_key, 6), dim), (shards_of,), jnp.float32, smallest / len(split), largest / len(split))
        return jnp.repeat(jnp.exp(draws), shape[dim] // shards_of).reshape((-1,) + (1,) * (len(shape) - dim - 1))

    loudness = one(*split[0])
    for cut in split[1:]:
        loudness = loudness * one(*cut)
    return loudness


def bell_draw(own_key, shape, spread, limit, shards=(), kind=jnp.bfloat16):
    drawn = jax.random.normal(own_key, shape, jnp.float32) * spread
    if len(shards) > 0:
        drawn = shard_levels(own_key, shape, shards, -0.22, 0.18) * drawn
    return jnp.clip(drawn, min=-limit, max=limit).astype(kind)


def setup_inputs(seed: int = 0) -> dict:
    streams_of = jax.random.split(jax.random.key(seed), 7)
    noisy_image = bell_draw(streams_of[0], (NZ, NY, NX), 1.0, 6.0, ((0, 4), (1, 2), (2, 4)), jnp.float32)
    fidelity = jnp.clip(jnp.exp(math.log(8.0) - 2.7725887 * jax.random.uniform(streams_of[1], (NZ, NY, NX), jnp.float32) ** shard_levels(streams_of[1], (NZ, NY, NX), ((0, 4), (1, 2), (2, 4)), -0.2, 0.2)), 0.5, 8.0)
    primal_u = bell_draw(streams_of[2], (NZ, NY, NX), 1.0, 6.0, ((0, 4), (1, 2), (2, 4)), jnp.float32)
    primal_v = bell_draw(streams_of[3], (3, NZ, NY, NX), 0.3, 2.0, ((1, 4), (2, 2), (3, 4)), jnp.float32)
    dual_p = bell_draw(streams_of[4], (3, NZ, NY, NX), 0.4, 2.5, ((1, 4), (2, 2), (3, 4)), jnp.float32)
    dual_q = bell_draw(streams_of[5], (6, NZ, NY, NX), 0.4, 2.5, ((1, 4), (2, 2), (3, 4)), jnp.float32)
    return {"noisy_image": noisy_image, "fidelity": fidelity, "primal_u": primal_u, "primal_v": primal_v, "dual_p": dual_p, "dual_q": dual_q}


first_alpha = 0.5
second_alpha = 1.0
dual_step = 0.2
primal_step = 0.2
index_pairs = ((0, 0), (1, 1), (2, 2), (0, 1), (0, 2), (1, 2))

def pair_index(left_axis, right_axis):
    for position, entry_pair in enumerate(index_pairs):
        if entry_pair == (left_axis, right_axis) or entry_pair == (right_axis, left_axis):
            return position
    return 0

def shift_next(values, axis_dim):
    extent = values.shape[axis_dim]
    tail_part = lax.slice_in_dim(values, 1, extent, axis=axis_dim)
    zeros_shape = list(values.shape)
    zeros_shape[axis_dim] = 1
    return jnp.concatenate([tail_part, jnp.zeros(zeros_shape, values.dtype)], axis=axis_dim)

def shift_prev(values, axis_dim):
    extent = values.shape[axis_dim]
    head_part = lax.slice_in_dim(values, 0, extent - 1, axis=axis_dim)
    zeros_shape = list(values.shape)
    zeros_shape[axis_dim] = 1
    return jnp.concatenate([jnp.zeros(zeros_shape, values.dtype), head_part], axis=axis_dim)

def edge_masks(extents):
    lower_masks = []
    upper_masks = []
    for component in range(3):
        extent = extents[2 - component]
        places = lax.iota(jnp.int32, extent)
        shape_list = [1, 1, 1, 1]
        shape_list[3 - component] = extent
        upper_masks.append((places < extent - 1).astype(jnp.float32).reshape(shape_list))
        lower_masks.append((places > 0).astype(jnp.float32).reshape(shape_list))
    return (lower_masks, upper_masks)

def q_rows(stacked, column):
    return jnp.stack([stacked[pair_index(row_axis, column)] for row_axis in range(3)], axis=0)

def project(stacked, weights, bound):
    magnitude = jnp.sqrt(lax.optimization_barrier(jnp.sum(weights * stacked * stacked, axis=0, keepdims=True)))
    return stacked / jnp.maximum(1.0, magnitude / bound)

def dual_update(bar_u, bar_v, grad_dual, sym_dual, next_u, prev_v, lower_masks, upper_masks):
    grads = jnp.concatenate([upper_masks[component] * (next_u[component] - bar_u) for component in range(3)], axis=0)
    trial_p = grad_dual + dual_step * (grads - bar_v)
    new_p = project(trial_p, jnp.ones((3, 1, 1, 1), jnp.float32), first_alpha)
    derivs = [lower_masks[component] * (bar_v - prev_v[component]) for component in range(3)]
    sym_parts = []
    for left_axis, right_axis in index_pairs:
        sym_parts.append(0.5 * (derivs[right_axis][left_axis] + derivs[left_axis][right_axis]))
    trial_q = sym_dual + dual_step * jnp.stack(sym_parts, axis=0)
    weights = jnp.array([1.0, 1.0, 1.0, 2.0, 2.0, 2.0], jnp.float32).reshape((6, 1, 1, 1))
    new_q = project(trial_q, weights, second_alpha)
    return (new_p, new_q)

def primal_update(image_u, vector_v, grad_dual, sym_dual, noisy, weight_map, prev_p, next_q, lower_masks, upper_masks):
    divergence = jnp.zeros_like(image_u)
    second_div = jnp.zeros_like(vector_v)
    for component in range(3):
        divergence = divergence + upper_masks[component] * grad_dual[component:component + 1] - prev_p[component]
        second_div = second_div + next_q[component] - lower_masks[component] * q_rows(sym_dual, component)
    new_u = (image_u + primal_step * divergence + primal_step * weight_map * noisy) / (1.0 + primal_step * weight_map)
    new_v = vector_v + primal_step * (grad_dual + second_div)
    return (new_u, new_v)

def reference(noisy_image, fidelity, primal_u, primal_v, dual_p, dual_q):
    noisy = noisy_image[None]
    weight_map = fidelity[None]
    image_u = primal_u[None]
    vector_v = primal_v
    grad_dual = dual_p
    sym_dual = dual_q
    lower_masks, upper_masks = edge_masks(noisy_image.shape)
    bar_u = image_u
    bar_v = vector_v
    for step_index in range(ITERS):
        next_u = [shift_next(bar_u, 3 - component) for component in range(3)]
        prev_v = [shift_prev(bar_v, 3 - component) for component in range(3)]
        grad_dual, sym_dual = dual_update(bar_u, bar_v, grad_dual, sym_dual, next_u, prev_v, lower_masks, upper_masks)
        prev_p = [shift_prev(grad_dual[component:component + 1], 3 - component) for component in range(3)]
        next_q = [shift_next(q_rows(sym_dual, component), 3 - component) for component in range(3)]
        new_u, new_v = primal_update(image_u, vector_v, grad_dual, sym_dual, noisy, weight_map, prev_p, next_q, lower_masks, upper_masks)
        bar_u = 2.0 * new_u - image_u
        bar_v = 2.0 * new_v - vector_v
        image_u = new_u
        vector_v = new_v
    return (image_u[0], vector_v, grad_dual, sym_dual)
```

```python
import functools
import itertools

import jax
import jax.numpy as jnp
from jax import lax
from jax.experimental import pallas as pl
from jax.experimental.pallas import tpu as pltpu
from jax.sharding import PartitionSpec as P

ITERS = 3
HALO = ITERS
ROW0 = 8
SLOT = 8
LANES = 128

first_alpha = 0.5
second_alpha = 1.0
dual_step = 0.2
primal_step = 0.2

AXES = ("gx", "gy", "gz")
FIELDS = 15
F, W, U, V, PF, QF = 0, 1, 2, 3, 6, 9
GROUPS = (FIELDS + 1) // 2


def spans(low):
    chosen = [(F, 2), (W, 2), (U, 3), (V, 3), (V + 1, 3), (V + 2, 3)]
    chosen += [(PF + i, 2 if low else 3) for i in range(3)]
    chosen += [(QF + i, 3 if low else 2) for i in range(6)]
    if not low:
        chosen += [(U, 3)]
    return [(field, 0 if low else -count, count) for field, count in chosen]


def entries(low):
    return [(field, first + i) for field, first, count in spans(low) for i in range(count)]


SENT = len(entries(True))


def colours(size):
    return ("even", "odd")[: min(size - 1, 2)]


def partner(place, colour, size):
    other = place ^ 1 if colour == "even" else ((place + 1) ^ 1) - 1
    return other if 0 <= other < size else None


def exchange(values, moves, sizes):
    pairs = []
    for place in itertools.product(*(range(sizes[axis]) for axis in AXES)):
        other = list(place)
        for axis, colour in moves.items():
            other[AXES.index(axis)] = partner(place[AXES.index(axis)], colour, sizes[axis])
        if None in other:
            spare = [axis for axis in AXES if axis not in moves and sizes[axis] % 2 == 0]
            if not spare:
                continue
            other = list(place)
            other[AXES.index(spare[0])] ^= 1
        source, target = 0, 0
        for axis, here, there in zip(AXES, place, other):
            source = source * sizes[axis] + here
            target = target * sizes[axis] + there
        pairs.append((source, target))
    return lax.ppermute(values, AXES, pairs)


def sends_low(colour, parity):
    return (colour == "even") == (parity == 1)


def colour_of(side, parity):
    return "even" if (side == "low") == (parity == 1) else "odd"


def pick(received, colour):
    return received.get(colour, received["even"])


def pack_z(extents, zs, pos, f, w, u, v, p, q, *rest):
    outs = dict(zip(zs, rest[: len(zs)]))
    sem = rest[len(zs)]
    nz = extents[0]

    def source(field, first, count):
        first = first % nz if first < 0 else first
        layers = pl.ds(first, count)
        if field < V:
            return (f, w, u)[field].at[layers]
        stacked, base = ((v, V), (p, PF), (q, QF))[(field >= PF) + (field >= QF)]
        return stacked.at[field - base, layers]

    for parity in (0, 1):

        @pl.when(pos[2] % 2 == parity)
        def _():
            copies = []
            for colour, out in outs.items():
                at = 0
                for field, first, count in spans(sends_low(colour, parity)):
                    copies.append(
                        pltpu.make_async_copy(source(field, first, count), out.at[pl.ds(at, count)], sem)
                    )
                    at += count
            for copy in copies:
                copy.start()
            for copy in copies:
                copy.wait()


def pack_own(extents, ys, zs, pos, f, w, u, v, p, q, ext, *rest):
    nz, ny, _ = extents
    rows = ny + 2 * ROW0
    combos = list(itertools.product(zs, ys))
    y_outs = dict(zip(ys, rest[: len(ys)]))
    yz_outs = dict(zip(combos, rest[len(ys) : len(ys) + len(combos)]))
    sem = rest[-1]
    own = (pl.ds(HALO, nz), pl.ds(ROW0, ny))
    copies = [
        pltpu.make_async_copy(array, ext.at[(field,) + own], sem)
        for field, array in ((F, f), (W, w), (U, u))
    ]
    copies += [
        pltpu.make_async_copy(array, ext.at[(pl.ds(field, count),) + own], sem)
        for field, array, count in ((V, v, 3), (PF, p, 3), (QF, q, 6))
    ]
    for copy in copies:
        copy.start()
    for copy in copies:
        copy.wait()
    flat = ext.reshape(FIELDS * (nz + 2 * HALO) * rows, LANES)

    def layer(side_layer, extent):
        return side_layer % extent

    for parity in (0, 1):

        @pl.when(pos[1] % 2 == parity)
        def _():
            for colour in ys:
                for i, (field, at) in enumerate(entries(sends_low(colour, parity))):
                    start = (field * (nz + 2 * HALO) + HALO) * rows + ROW0 + layer(at, ny)
                    y_outs[colour][i] = flat[pl.ds(start, nz, stride=rows), :]

    for z_parity, y_parity in itertools.product((0, 1), (0, 1)):

        @pl.when(jnp.logical_and(pos[2] % 2 == z_parity, pos[1] % 2 == y_parity))
        def _():
            for z_colour, y_colour in combos:
                first_row = ROW0 + (0 if sends_low(y_colour, y_parity) else ny - HALO)
                for i, (field, at) in enumerate(entries(sends_low(z_colour, z_parity))):
                    yz_outs[z_colour, y_colour][pl.ds(i * HALO, HALO), :] = ext[
                        field, HALO + layer(at, nz), pl.ds(first_row, HALO), :
                    ]


def tile_starts(ny):
    return [ROW0 - HALO + 8 * i for i in range(-(-(ny + 2 * HALO) // 8))]


def join_halo(extents, xs, ys, zs, pos, ext_in, *rest):
    del ext_in
    nz, ny, _ = extents
    rows = ny + 2 * ROW0
    levels = nz + 2 * HALO
    combos = list(itertools.product(zs, ys))
    z_got = dict(zip(zs, rest))
    rest = rest[len(zs) :]
    y_got = dict(zip(ys, rest))
    rest = rest[len(ys) :]
    yz_got = dict(zip(combos, rest))
    rest = rest[len(combos) :]
    ext, strip = rest[:2]
    x_outs = dict(zip(xs, rest[2:]))
    flat = ext.reshape(FIELDS * levels * rows, LANES)

    def placed(side, extent):
        if side == "low":
            return entries(False)
        return [(field, extent + at) for field, at in entries(True)]

    if zs:
        for parity in (0, 1):

            @pl.when(pos[2] % 2 == parity)
            def _():
                for side in ("low", "high"):
                    got = pick(z_got, colour_of(side, parity))
                    for i, (field, at) in list(enumerate(placed(side, nz)))[::-1]:
                        ext[field, HALO + at, pl.ds(ROW0, ny), :] = got[i]

    if ys:
        for parity in (0, 1):

            @pl.when(pos[1] % 2 == parity)
            def _():
                for side in ("low", "high"):
                    got = pick(y_got, colour_of(side, parity))
                    for i, (field, at) in list(enumerate(placed(side, ny)))[::-1]:
                        start = (field * levels + HALO) * rows + ROW0 + at
                        flat[pl.ds(start, nz, stride=rows), :] = got[i]

    if combos:
        for z_parity, y_parity in itertools.product((0, 1), (0, 1)):

            @pl.when(jnp.logical_and(pos[2] % 2 == z_parity, pos[1] % 2 == y_parity))
            def _():
                for z_side, y_side in itertools.product(("low", "high"), ("low", "high")):
                    z_colour, y_colour = colour_of(z_side, z_parity), colour_of(y_side, y_parity)
                    z_colour = z_colour if z_colour in zs else "even"
                    y_colour = y_colour if y_colour in ys else "even"
                    got = yz_got[z_colour, y_colour]
                    row = ROW0 + (-HALO if y_side == "low" else ny)
                    for i, (field, at) in list(enumerate(placed(z_side, nz)))[::-1]:
                        ext[field, HALO + at, pl.ds(row, HALO), :] = got[pl.ds(i * HALO, HALO), :]

    lane = lax.broadcasted_iota(jnp.int32, (8, LANES), 1)
    for row in tile_starts(ny):

        def gather(field, carry):
            total = jnp.zeros((8, LANES), jnp.float32)
            for level in range(levels):
                turned = pltpu.roll(ext[field, level, pl.ds(row, 8), :], level * SLOT + HALO, 1)
                here = lane < (level + 1) * SLOT
                total = jnp.where(jnp.logical_and(here, lane >= level * SLOT), turned, total)
            strip[field, pl.ds(row, 8), :] = total
            return carry

        lax.fori_loop(0, FIELDS, gather, 0)

    slot = lane % SLOT
    for colour in xs:
        low = (pos[0] % 2 == 1) if colour == "even" else (pos[0] % 2 == 0)
        turn = jnp.where(low, LANES - 3, 4)
        keep = jnp.where(low, slot - 3, 3 - slot) >= 0
        for group, row in itertools.product(range(GROUPS), tile_starts(ny)):
            mine = strip[2 * group, pl.ds(row, 8), :]
            if 2 * group + 1 < FIELDS:
                other = pltpu.roll(strip[2 * group + 1, pl.ds(row, 8), :], turn, 1)
                mine = jnp.where(keep, mine, other)
            x_outs[colour][group, pl.ds(row - tile_starts(ny)[0], 8), :] = mine


def shrink(total, bound):
    return lax.rsqrt(jnp.maximum(1.0, total * (1.0 / (bound * bound))))


def dual_step_of(bar, next_bar, prev_bar, p, q, upper, lower):
    t = [p[a] + upper[a] * (next_bar[a] - bar[0]) - bar[1 + a] for a in range(3)]
    scale = shrink(t[0] * t[0] + t[1] * t[1] + t[2] * t[2], first_alpha)
    d = [[lower[b] * (bar[1 + a] - prev_bar[b][a]) for a in range(3)] for b in range(3)]
    s = [q[a] + d[a][a] for a in range(3)]
    for i, (a, b) in enumerate(((0, 1), (0, 2), (1, 2))):
        s.append(q[3 + i] + 0.5 * (d[b][a] + d[a][b]))
    off = s[3] * s[3] + s[4] * s[4] + s[5] * s[5]
    q_scale = shrink(s[0] * s[0] + s[1] * s[1] + s[2] * s[2] + (off + off), second_alpha)
    return [value * scale for value in t], [value * q_scale for value in s]


ROWS_OF_Q = ((0, 3, 4), (3, 1, 5), (4, 5, 2))


def primal_step_of(u, v, a_map, b_map, p, q, prev_p, next_q, upper, lower):
    div = None
    for a in range(3):
        term = upper[a] * p[a] - lower[a] * prev_p[a]
        div = term if div is None else div + term
    new_u = (u + primal_step * div) * b_map + a_map
    new_v = []
    for a in range(3):
        total = p[a]
        for b in range(3):
            total = total + (upper[b] * next_q[b][a] - lower[b] * q[ROWS_OF_Q[b][a]])
        new_v.append(v[a] + primal_step * total)
    bar = [(2.0 * dual_step) * new_u - dual_step * u]
    bar += [(2.0 * dual_step) * new_v[a] - dual_step * v[a] for a in range(3)]
    return new_u, new_v, bar


def solve(extents, sizes, xs, pos, ext_in, strip_in, *rest):
    del ext_in
    nz, ny, nx = extents
    rows = ny + 2 * ROW0
    levels = nz + 2 * HALO
    x_got = dict(zip(xs, rest[: len(xs)]))
    ext, out_u, out_v, out_p, out_q, side, bars, side_bars, sem = rest[len(xs) :]
    starts = tile_starts(ny)
    lane = lax.broadcasted_iota(jnp.int32, (8, LANES), 1)
    sub = lax.broadcasted_iota(jnp.int32, (8, LANES), 0)
    slot = lane % SLOT
    f32 = jnp.float32

    def masks(places, full):
        upper = jnp.logical_and(places >= 0, places < full - 1)
        lower = jnp.logical_and(places > 0, places < full)
        return upper.astype(f32), lower.astype(f32)

    full = [sizes[axis] * extent for axis, extent in zip(AXES, (nx, ny, nz))]
    y_masks = [masks(pos[1] * ny + (row - ROW0) + sub, full[1]) for row in starts]
    x_main = masks(pos[0] * nx + lane, full[0])
    x_side = [masks(pos[0] * nx + first + slot, full[0]) for first in (-HALO, nx - HALO)]
    z_side = masks(pos[2] * nz - HALO + lane // SLOT, full[2])

    def z_main(level):
        place = pos[2] * nz - HALO + level
        upper = jnp.where(jnp.logical_and(place >= 0, place < full[2] - 1), 1.0, 0.0)
        lower = jnp.where(jnp.logical_and(place > 0, place < full[2]), 1.0, 0.0)
        return upper.astype(f32), lower.astype(f32)

    def fill(got_low, got_high):
        for field, (i, row) in itertools.product(range(FIELDS), enumerate(starts)):
            own = strip_in[field, pl.ds(row, 8), :]
            at = (field // 2, pl.ds(8 * i, 8), slice(None))
            low, high = got_low[at], got_high[at]
            if field % 2:
                low, high = pltpu.roll(low, LANES - 4, 1), pltpu.roll(high, 3, 1)
            side[field, 0, pl.ds(row, 8), :] = jnp.where(slot < HALO, low, own)
            side[field, 1, pl.ds(row, 8), :] = jnp.where(slot < HALO, own, high)

    for parity in (0, 1):

        @pl.when(pos[0] % 2 == parity)
        def _():
            fill(pick(x_got, colour_of("low", parity)), pick(x_got, colour_of("high", parity)))

    def prepare(load, store, store_bar):
        f, w = load(F), load(W)
        inverse = 1.0 / (1.0 + primal_step * w)
        store(F, (primal_step * w * f) * inverse)
        store(W, inverse)
        for a in range(4):
            store_bar(a, dual_step * load(U + a))

    def main_refs(level, row):
        at = (level, pl.ds(row, 8), slice(None))

        def load(field):
            return ext[(field,) + at]

        def store(field, value):
            ext[(field,) + at] = value

        def store_bar(a, value):
            bars[a, level + 1, pl.ds(row, 8), :] = value

        return load, store, store_bar

    def side_refs(which, row):
        at = (which, pl.ds(row, 8), slice(None))

        def load(field):
            return side[(field,) + at]

        def store(field, value):
            side[(field,) + at] = value

        def store_bar(a, value):
            side_bars[(a,) + at] = value

        return load, store, store_bar

    def prepare_level(level, carry):
        for row in starts:
            prepare(*main_refs(level, row))
        return carry

    for which, row in itertools.product((0, 1), starts):
        prepare(*side_refs(which, row))
    lax.fori_loop(0, levels, prepare_level, 0)

    first, last = lane == 0, lane == LANES - 1

    def from_low(values, level):
        return pltpu.roll(values, LANES - HALO + 1 - SLOT * level, 1)

    def from_high(values, level):
        return pltpu.roll(values, LANES - 1 - HALO - SLOT * level, 1)

    def dual_main(level, carry):
        z_upper, z_lower = z_main(level)
        for (i, row) in enumerate(starts):
            load, store, _ = main_refs(level, row)
            here = pl.ds(row, 8)
            bar = [bars[a, level + 1, here, :] for a in range(4)]
            edge = from_high(side_bars[0, 1, here, :], level)
            next_bar = [
                jnp.where(last, edge, pltpu.roll(bar[0], LANES - 1, 1)),
                bars[0, level + 1, pl.ds(row + 1, 8), :],
                bars[0, level + 2, here, :],
            ]
            prev_bar = [
                [
                    jnp.where(
                        first,
                        from_low(side_bars[1 + a, 0, here, :], level),
                        pltpu.roll(bar[1 + a], 1, 1),
                    )
                    for a in range(3)
                ],
                [bars[1 + a, level + 1, pl.ds(row - 1, 8), :] for a in range(3)],
                [bars[1 + a, level, here, :] for a in range(3)],
            ]
            p, q = dual_step_of(
                bar,
                next_bar,
                prev_bar,
                [load(PF + a) for a in range(3)],
                [load(QF + a) for a in range(6)],
                (x_main[0], y_masks[i][0], z_upper),
                (x_main[1], y_masks[i][1], z_lower),
            )
            for a in range(3):
                store(PF + a, p[a])
            for a in range(6):
                store(QF + a, q[a])
        return carry

    def primal_main(level, carry):
        z_upper, z_lower = z_main(level)
        for (i, row) in enumerate(starts):
            load, store, store_bar = main_refs(level, row)
            here = pl.ds(row, 8)
            p = [load(PF + a) for a in range(3)]
            q = [load(QF + a) for a in range(6)]
            prev_p = [
                jnp.where(first, from_low(side[PF, 0, here, :], level), pltpu.roll(p[0], 1, 1)),
                ext[PF + 1, level, pl.ds(row - 1, 8), :],
                ext[PF + 2, level - 1, here, :],
            ]
            next_q = [
                [
                    jnp.where(
                        last,
                        from_high(side[QF + j, 1, here, :], level),
                        pltpu.roll(q[j], LANES - 1, 1),
                    )
                    for j in ROWS_OF_Q[0]
                ],
                [ext[QF + j, level, pl.ds(row + 1, 8), :] for j in ROWS_OF_Q[1]],
                [ext[QF + j, level + 1, here, :] for j in ROWS_OF_Q[2]],
            ]
            new_u, new_v, bar = primal_step_of(
                load(U),
                [load(V + a) for a in range(3)],
                load(F),
                load(W),
                p,
                q,
                prev_p,
                next_q,
                (x_main[0], y_masks[i][0], z_upper),
                (x_main[1], y_masks[i][1], z_lower),
            )
            for a, value in enumerate([new_u] + new_v):
                store(U + a, value)
            for a in range(4):
                store_bar(a, bar[a])
        return carry

    def dual_side(which):
        updates = []
        for (i, row) in enumerate(starts):
            load, _, _ = side_refs(which, row)
            here = pl.ds(row, 8)
            bar = [side_bars[a, which, here, :] for a in range(4)]
            next_bar = [
                pltpu.roll(bar[0], LANES - 1, 1),
                side_bars[0, which, pl.ds(row + 1, 8), :],
                pltpu.roll(bar[0], LANES - SLOT, 1),
            ]
            prev_bar = [
                [pltpu.roll(bar[1 + a], 1, 1) for a in range(3)],
                [side_bars[1 + a, which, pl.ds(row - 1, 8), :] for a in range(3)],
                [pltpu.roll(bar[1 + a], SLOT, 1) for a in range(3)],
            ]
            p, q = dual_step_of(
                bar,
                next_bar,
                prev_bar,
                [load(PF + a) for a in range(3)],
                [load(QF + a) for a in range(6)],
                (x_side[which][0], y_masks[i][0], z_side[0]),
                (x_side[which][1], y_masks[i][1], z_side[1]),
            )
            for a, value in enumerate(p + q):
                side[PF + a, which, here, :] = value

    def primal_side(which):
        for (i, row) in enumerate(starts):
            load, store, store_bar = side_refs(which, row)
            here = pl.ds(row, 8)
            p = [load(PF + a) for a in range(3)]
            q = [load(QF + a) for a in range(6)]
            prev_p = [
                pltpu.roll(p[0], 1, 1),
                side[PF + 1, which, pl.ds(row - 1, 8), :],
                pltpu.roll(p[2], SLOT, 1),
            ]
            next_q = [
                [pltpu.roll(q[j], LANES - 1, 1) for j in ROWS_OF_Q[0]],
                [side[QF + j, which, pl.ds(row + 1, 8), :] for j in ROWS_OF_Q[1]],
                [pltpu.roll(q[j], LANES - SLOT, 1) for j in ROWS_OF_Q[2]],
            ]
            new_u, new_v, bar = primal_step_of(
                load(U),
                [load(V + a) for a in range(3)],
                load(F),
                load(W),
                p,
                q,
                prev_p,
                next_q,
                (x_side[which][0], y_masks[i][0], z_side[0]),
                (x_side[which][1], y_masks[i][1], z_side[1]),
            )
            for a, value in enumerate([new_u] + new_v):
                store(U + a, value)
            for a in range(4):
                store_bar(a, bar[a])

    def out_copies(fields):
        own = (pl.ds(HALO, nz), pl.ds(ROW0, ny))
        return [
            pltpu.make_async_copy(ext.at[(field,) + own], out, sem) for field, out in fields
        ]

    duals = [(pl.ds(PF, 3), out_p), (pl.ds(QF, 6), out_q)]
    primals = [(U, out_u), (pl.ds(V, 3), out_v)]

    def iteration(step, carry):
        lax.fori_loop(step, levels - step, dual_main, 0)
        for which in (0, 1):
            dual_side(which)

        @pl.when(step == ITERS - 1)
        def _():
            for copy in out_copies(duals):
                copy.start()

        lax.fori_loop(step + 1, levels - 1 - step, primal_main, 0)
        for which in (0, 1):
            primal_side(which)
        return carry

    lax.fori_loop(0, ITERS, iteration, 0)
    for copy in out_copies(primals):
        copy.start()
    for copy in out_copies(duals + primals):
        copy.wait()


def per_device(sizes, noisy_image, fidelity, primal_u, primal_v, dual_p, dual_q):
    nz, ny, nx = extents = noisy_image.shape
    levels, rows = nz + 2 * HALO, ny + 2 * ROW0
    assert nx == LANES and ny % 8 == 0 and levels * SLOT <= LANES
    assert min(nz, ny) >= HALO
    xs, ys, zs = (colours(sizes[axis]) for axis in AXES)
    combos = list(itertools.product(zs, ys))
    pos = jnp.stack([lax.axis_index(axis) for axis in AXES])
    args = (noisy_image, fidelity, primal_u, primal_v, dual_p, dual_q)
    f32 = jnp.float32
    smem = pl.BlockSpec(memory_space=pltpu.SMEM)
    anywhere = pl.BlockSpec(memory_space=pl.ANY)
    vmem = pl.BlockSpec(memory_space=pltpu.VMEM)

    def shaped(*shape):
        return jax.ShapeDtypeStruct(shape, f32)

    def call(body, ins, outs, out_specs, name, limit, **more):
        return pl.pallas_call(
            body,
            in_specs=ins,
            out_specs=out_specs,
            out_shape=outs,
            name=name,
            compiler_params=pltpu.CompilerParams(vmem_limit_bytes=limit * 1024 * 1024),
            **more,
        )

    z_pay = call(
        functools.partial(pack_z, extents, zs),
        [smem] + [anywhere] * 6,
        [shaped(SENT, ny, nx)] * len(zs),
        [vmem] * len(zs),
        "pack_z",
        8,
        scratch_shapes=[pltpu.SemaphoreType.DMA],
    )(pos, *args)
    z_got = [exchange(pay, {"gz": c}, sizes) for c, pay in zip(zs, z_pay)]

    strip_rows = 8 * len(tile_starts(ny))
    ext_shape = shaped(FIELDS, levels, rows, nx)
    own = call(
        functools.partial(pack_own, extents, ys, zs),
        [smem] + [anywhere] * 6,
        [ext_shape]
        + [shaped(SENT, nz, nx)] * len(ys)
        + [shaped(SENT * HALO, nx)] * len(combos),
        [vmem] * (1 + len(ys) + len(combos)),
        "pack_own",
        16,
        scratch_shapes=[pltpu.SemaphoreType.DMA],
    )(pos, *args)
    ext, y_pay, yz_pay = own[0], own[1 : 1 + len(ys)], own[1 + len(ys) :]
    yz_got = [exchange(pay, {"gz": a, "gy": b}, sizes) for (a, b), pay in zip(combos, yz_pay)]
    y_got = [exchange(pay, {"gy": c}, sizes) for c, pay in zip(ys, y_pay)]

    joined = call(
        functools.partial(join_halo, extents, xs, ys, zs),
        [smem] + [vmem] * (1 + len(zs) + len(ys) + len(combos)),
        [ext_shape, shaped(FIELDS, rows, nx)] + [shaped(GROUPS, strip_rows, nx)] * len(xs),
        [vmem] * (2 + len(xs)),
        "join_halo",
        20,
        input_output_aliases={1: 0},
    )(pos, ext, *z_got, *y_got, *yz_got)
    ext, strip, x_pay = joined[0], joined[1], joined[2:]
    x_got = [exchange(pay, {"gx": c}, sizes) for c, pay in zip(xs, x_pay)]

    solved = call(
        functools.partial(solve, extents, sizes, xs),
        [smem] + [vmem] * (2 + len(xs)),
        [ext_shape] + [shaped(*a.shape) for a in (primal_u, primal_v, dual_p, dual_q)],
        [vmem] + [anywhere] * 4,
        "solve",
        24,
        input_output_aliases={1: 0},
        scratch_shapes=[
            pltpu.VMEM((FIELDS, 2, rows, nx), f32),
            pltpu.VMEM((4, levels + 2, rows, nx), f32),
            pltpu.VMEM((4, 2, rows, nx), f32),
            pltpu.SemaphoreType.DMA,
        ],
    )(pos, ext, strip, *x_got)
    return tuple(solved[1:])


def solution(mesh):
    sizes = {axis: mesh.shape[axis] for axis in AXES}
    scalar, stacked = P("gz", "gy", "gx"), P(None, "gz", "gy", "gx")
    return jax.shard_map(
        functools.partial(per_device, sizes),
        mesh=mesh,
        in_specs=(scalar,) * 3 + (stacked,) * 3,
        out_specs=(scalar,) + (stacked,) * 3,
        check_vma=False,
    )
```

```python
import functools
import itertools

import jax
import jax.numpy as jnp
from jax import lax
from jax.experimental import pallas as pl
from jax.experimental.pallas import tpu as pltpu
from jax.sharding import PartitionSpec as P

ITERS = 3
HALO = ITERS
ROW0 = 8
SLOT = 8
LANES = 128

first_alpha = 0.5
second_alpha = 1.0
dual_step = 0.2
primal_step = 0.2

AXES = ("gx", "gy", "gz")
FIELDS = 15
F, W, U, V, PF, QF = 0, 1, 2, 3, 6, 9
GROUPS = (FIELDS + 1) // 2


def spans(low):
    chosen = [(F, 2), (W, 2), (U, 3), (V, 3), (V + 1, 3), (V + 2, 3)]
    chosen += [(PF + i, 2 if low else 3) for i in range(3)]
    chosen += [(QF + i, 3 if low else 2) for i in range(6)]
    if not low:
        chosen += [(U, 3)]
    return [(field, 0 if low else -count, count) for field, count in chosen]


def entries(low):
    return [(field, first + i) for field, first, count in spans(low) for i in range(count)]


SENT = len(entries(True))


def colours(size):
    return ("even", "odd")[: min(size - 1, 2)]


def partner(place, colour, size):
    other = place ^ 1 if colour == "even" else ((place + 1) ^ 1) - 1
    return other if 0 <= other < size else None


def exchange(values, moves, sizes):
    pairs = []
    for place in itertools.product(*(range(sizes[axis]) for axis in AXES)):
        other = list(place)
        for axis, colour in moves.items():
            other[AXES.index(axis)] = partner(place[AXES.index(axis)], colour, sizes[axis])
        if None in other:
            spare = [axis for axis in AXES if axis not in moves and sizes[axis] % 2 == 0]
            if not spare:
                continue
            other = list(place)
            other[AXES.index(spare[0])] ^= 1
        source, target = 0, 0
        for axis, here, there in zip(AXES, place, other):
            source = source * sizes[axis] + here
            target = target * sizes[axis] + there
        pairs.append((source, target))
    return lax.ppermute(values, AXES, pairs)


def sends_low(colour, parity):
    return (colour == "even") == (parity == 1)


def colour_of(side, parity):
    return "even" if (side == "low") == (parity == 1) else "odd"


def pick(received, colour):
    return received.get(colour, received["even"])


def pack_z(extents, zs, pos, f, w, u, v, p, q, *rest):
    outs = dict(zip(zs, rest[: len(zs)]))
    sem = rest[len(zs)]
    nz = extents[0]

    def source(field, first, count):
        first = first % nz if first < 0 else first
        layers = pl.ds(first, count)
        if field < V:
            return (f, w, u)[field].at[layers]
        stacked, base = ((v, V), (p, PF), (q, QF))[(field >= PF) + (field >= QF)]
        return stacked.at[field - base, layers]

    for parity in (0, 1):

        @pl.when(pos[2] % 2 == parity)
        def _():
            copies = []
            for colour, out in outs.items():
                at = 0
                for field, first, count in spans(sends_low(colour, parity)):
                    copies.append(
                        pltpu.make_async_copy(source(field, first, count), out.at[pl.ds(at, count)], sem)
                    )
                    at += count
            for copy in copies:
                copy.start()
            for copy in copies:
                copy.wait()


def pack_own(extents, ys, zs, pos, f, w, u, v, p, q, ext, *rest):
    nz, ny, _ = extents
    rows = ny + 2 * ROW0
    combos = list(itertools.product(zs, ys))
    y_outs = dict(zip(ys, rest[: len(ys)]))
    yz_outs = dict(zip(combos, rest[len(ys) : len(ys) + len(combos)]))
    sem = rest[-1]
    own = (pl.ds(HALO, nz), pl.ds(ROW0, ny))
    copies = [
        pltpu.make_async_copy(array, ext.at[(field,) + own], sem)
        for field, array in ((F, f), (W, w), (U, u))
    ]
    copies += [
        pltpu.make_async_copy(array, ext.at[(pl.ds(field, count),) + own], sem)
        for field, array, count in ((V, v, 3), (PF, p, 3), (QF, q, 6))
    ]
    for copy in copies:
        copy.start()
    for copy in copies:
        copy.wait()
    flat = ext.reshape(FIELDS * (nz + 2 * HALO) * rows, LANES)

    def layer(side_layer, extent):
        return side_layer % extent

    for parity in (0, 1):

        @pl.when(pos[1] % 2 == parity)
        def _():
            for colour in ys:
                for i, (field, at) in enumerate(entries(sends_low(colour, parity))):
                    start = (field * (nz + 2 * HALO) + HALO) * rows + ROW0 + layer(at, ny)
                    y_outs[colour][i] = flat[pl.ds(start, nz, stride=rows), :]

    for z_parity, y_parity in itertools.product((0, 1), (0, 1)):

        @pl.when(jnp.logical_and(pos[2] % 2 == z_parity, pos[1] % 2 == y_parity))
        def _():
            for z_colour, y_colour in combos:
                first_row = ROW0 + (0 if sends_low(y_colour, y_parity) else ny - HALO)
                for i, (field, at) in enumerate(entries(sends_low(z_colour, z_parity))):
                    yz_outs[z_colour, y_colour][pl.ds(i * HALO, HALO), :] = ext[
                        field, HALO + layer(at, nz), pl.ds(first_row, HALO), :
                    ]


def tile_starts(ny):
    return [ROW0 - HALO + 8 * i for i in range(-(-(ny + 2 * HALO) // 8))]


def join_halo(extents, xs, ys, zs, pos, ext_in, *rest):
    del ext_in
    nz, ny, _ = extents
    rows = ny + 2 * ROW0
    levels = nz + 2 * HALO
    combos = list(itertools.product(zs, ys))
    z_got = dict(zip(zs, rest))
    rest = rest[len(zs) :]
    y_got = dict(zip(ys, rest))
    rest = rest[len(ys) :]
    yz_got = dict(zip(combos, rest))
    rest = rest[len(combos) :]
    ext, strip = rest[:2]
    x_outs = dict(zip(xs, rest[2:]))
    flat = ext.reshape(FIELDS * levels * rows, LANES)

    def placed(side, extent):
        if side == "low":
            return entries(False)
        return [(field, extent + at) for field, at in entries(True)]

    if zs:
        for parity in (0, 1):

            @pl.when(pos[2] % 2 == parity)
            def _():
                for side in ("low", "high"):
                    got = pick(z_got, colour_of(side, parity))
                    for i, (field, at) in list(enumerate(placed(side, nz)))[::-1]:
                        ext[field, HALO + at, pl.ds(ROW0, ny), :] = got[i]

    if ys:
        for parity in (0, 1):

            @pl.when(pos[1] % 2 == parity)
            def _():
                for side in ("low", "high"):
                    got = pick(y_got, colour_of(side, parity))
                    for i, (field, at) in list(enumerate(placed(side, ny)))[::-1]:
                        start = (field * levels + HALO) * rows + ROW0 + at
                        flat[pl.ds(start, nz, stride=rows), :] = got[i]

    if combos:
        for z_parity, y_parity in itertools.product((0, 1), (0, 1)):

            @pl.when(jnp.logical_and(pos[2] % 2 == z_parity, pos[1] % 2 == y_parity))
            def _():
                for z_side, y_side in itertools.product(("low", "high"), ("low", "high")):
                    z_colour, y_colour = colour_of(z_side, z_parity), colour_of(y_side, y_parity)
                    z_colour = z_colour if z_colour in zs else "even"
                    y_colour = y_colour if y_colour in ys else "even"
                    got = yz_got[z_colour, y_colour]
                    row = ROW0 + (-HALO if y_side == "low" else ny)
                    for i, (field, at) in list(enumerate(placed(z_side, nz)))[::-1]:
                        ext[field, HALO + at, pl.ds(row, HALO), :] = got[pl.ds(i * HALO, HALO), :]

    lane = lax.broadcasted_iota(jnp.int32, (8, LANES), 1)
    def gather(field, carry):
        for row in tile_starts(ny):
            total = jnp.zeros((8, LANES), jnp.float32)
            for level in range(levels):
                turned = pltpu.roll(ext[field, level, pl.ds(row, 8), :], level * SLOT + HALO, 1)
                total = jnp.where(lane >= level * SLOT, turned, total)
            strip[field, pl.ds(row, 8), :] = total
        return carry

    lax.fori_loop(0, FIELDS, gather, 0)

    slot = lane % SLOT
    for colour in xs:
        low = (pos[0] % 2 == 1) if colour == "even" else (pos[0] % 2 == 0)
        turn = jnp.where(low, LANES - 3, 4)
        keep = jnp.where(low, slot - 3, 3 - slot) >= 0
        for group, row in itertools.product(range(GROUPS), tile_starts(ny)):
            mine = strip[2 * group, pl.ds(row, 8), :]
            if 2 * group + 1 < FIELDS:
                other = pltpu.roll(strip[2 * group + 1, pl.ds(row, 8), :], turn, 1)
                mine = jnp.where(keep, mine, other)
            x_outs[colour][group, pl.ds(row - tile_starts(ny)[0], 8), :] = mine


def shrink(total, bound):
    return lax.rsqrt(jnp.maximum(1.0, total * (1.0 / (bound * bound))))


def dual_step_of(bar, next_bar, prev_bar, p, q, upper, lower):
    t = [p[a] + upper[a] * (next_bar[a] - bar[0]) - bar[1 + a] for a in range(3)]
    scale = shrink(t[0] * t[0] + t[1] * t[1] + t[2] * t[2], first_alpha)
    d = [[lower[b] * (bar[1 + a] - prev_bar[b][a]) for a in range(3)] for b in range(3)]
    s = [q[a] + d[a][a] for a in range(3)]
    for i, (a, b) in enumerate(((0, 1), (0, 2), (1, 2))):
        s.append(q[3 + i] + 0.5 * (d[b][a] + d[a][b]))
    off = s[3] * s[3] + s[4] * s[4] + s[5] * s[5]
    q_scale = shrink(s[0] * s[0] + s[1] * s[1] + s[2] * s[2] + (off + off), second_alpha)
    return [value * scale for value in t], [value * q_scale for value in s]


ROWS_OF_Q = ((0, 3, 4), (3, 1, 5), (4, 5, 2))


def primal_step_of(u, v, a_map, b_map, p, q, prev_p, next_q, upper, lower):
    div = None
    for a in range(3):
        term = upper[a] * p[a] - lower[a] * prev_p[a]
        div = term if div is None else div + term
    new_u = (u + primal_step * div) * b_map + a_map
    new_v = []
    for a in range(3):
        total = p[a]
        for b in range(3):
            total = total + (upper[b] * next_q[b][a] - lower[b] * q[ROWS_OF_Q[b][a]])
        new_v.append(v[a] + primal_step * total)
    bar = [(2.0 * dual_step) * new_u - dual_step * u]
    bar += [(2.0 * dual_step) * new_v[a] - dual_step * v[a] for a in range(3)]
    return new_u, new_v, bar


def solve(extents, sizes, xs, pos, ext_in, strip_in, *rest):
    del ext_in
    nz, ny, nx = extents
    rows = ny + 2 * ROW0
    levels = nz + 2 * HALO
    x_got = dict(zip(xs, rest[: len(xs)]))
    ext, out_u, out_v, out_p, out_q, side, bars, side_bars, sem = rest[len(xs) :]
    starts = tile_starts(ny)
    lane = lax.broadcasted_iota(jnp.int32, (8, LANES), 1)
    sub = lax.broadcasted_iota(jnp.int32, (8, LANES), 0)
    slot = lane % SLOT
    f32 = jnp.float32

    def masks(places, full):
        upper = jnp.logical_and(places >= 0, places < full - 1)
        lower = jnp.logical_and(places > 0, places < full)
        return upper.astype(f32), lower.astype(f32)

    full = [sizes[axis] * extent for axis, extent in zip(AXES, (nx, ny, nz))]
    y_masks = [masks(pos[1] * ny + (row - ROW0) + sub, full[1]) for row in starts]
    x_main = masks(pos[0] * nx + lane, full[0])
    x_side = [masks(pos[0] * nx + first + slot, full[0]) for first in (-HALO, nx - HALO)]
    z_side = masks(pos[2] * nz - HALO + lane // SLOT, full[2])

    def z_main(level):
        place = pos[2] * nz - HALO + level
        upper = jnp.where(jnp.logical_and(place >= 0, place < full[2] - 1), 1.0, 0.0)
        lower = jnp.where(jnp.logical_and(place > 0, place < full[2]), 1.0, 0.0)
        return upper.astype(f32), lower.astype(f32)

    def fill(got_low, got_high):
        for field, (i, row) in itertools.product(range(FIELDS), enumerate(starts)):
            own = strip_in[field, pl.ds(row, 8), :]
            at = (field // 2, pl.ds(8 * i, 8), slice(None))
            low, high = got_low[at], got_high[at]
            if field % 2:
                low, high = pltpu.roll(low, LANES - 4, 1), pltpu.roll(high, 3, 1)
            side[field, 0, pl.ds(row, 8), :] = jnp.where(slot < HALO, low, own)
            side[field, 1, pl.ds(row, 8), :] = jnp.where(slot < HALO, own, high)

    for parity in (0, 1):

        @pl.when(pos[0] % 2 == parity)
        def _():
            fill(pick(x_got, colour_of("low", parity)), pick(x_got, colour_of("high", parity)))

    def prepare(load, store, store_bar):
        f, w = load(F), load(W)
        inverse = 1.0 / (1.0 + primal_step * w)
        store(F, (primal_step * w * f) * inverse)
        store(W, inverse)
        for a in range(4):
            store_bar(a, dual_step * load(U + a))

    def main_refs(level, row):
        at = (level, pl.ds(row, 8), slice(None))

        def load(field):
            return ext[(field,) + at]

        def store(field, value):
            ext[(field,) + at] = value

        def store_bar(a, value):
            bars[a, level + 1, pl.ds(row, 8), :] = value

        return load, store, store_bar

    def side_refs(which, row):
        at = (which, pl.ds(row, 8), slice(None))

        def load(field):
            return side[(field,) + at]

        def store(field, value):
            side[(field,) + at] = value

        def store_bar(a, value):
            side_bars[(a,) + at] = value

        return load, store, store_bar

    def paired_loop(start, stop, body):
        many = 2 if levels % 2 == 0 else 1

        def trip(i, carry):
            for j in range(many):
                body(start + many * i + j, carry)
            return carry

        lax.fori_loop(0, (stop - start) // many, trip, 0)

    def prepare_level(level, carry):
        for row in starts:
            prepare(*main_refs(level, row))
        return carry

    for which, row in itertools.product((0, 1), starts):
        prepare(*side_refs(which, row))
    paired_loop(0, levels, prepare_level)

    first, last = lane == 0, lane == LANES - 1

    def from_low(values, level):
        return pltpu.roll(values, LANES - HALO + 1 - SLOT * level, 1)

    def from_high(values, level):
        return pltpu.roll(values, LANES - 1 - HALO - SLOT * level, 1)

    def dual_main(level, carry):
        z_upper, z_lower = z_main(level)
        for (i, row) in enumerate(starts):
            load, store, _ = main_refs(level, row)
            here = pl.ds(row, 8)
            bar = [bars[a, level + 1, here, :] for a in range(4)]
            edge = from_high(side_bars[0, 1, here, :], level)
            next_bar = [
                jnp.where(last, edge, pltpu.roll(bar[0], LANES - 1, 1)),
                bars[0, level + 1, pl.ds(row + 1, 8), :],
                bars[0, level + 2, here, :],
            ]
            prev_bar = [
                [
                    jnp.where(
                        first,
                        from_low(side_bars[1 + a, 0, here, :], level),
                        pltpu.roll(bar[1 + a], 1, 1),
                    )
                    for a in range(3)
                ],
                [bars[1 + a, level + 1, pl.ds(row - 1, 8), :] for a in range(3)],
                [bars[1 + a, level, here, :] for a in range(3)],
            ]
            p, q = dual_step_of(
                bar,
                next_bar,
                prev_bar,
                [load(PF + a) for a in range(3)],
                [load(QF + a) for a in range(6)],
                (x_main[0], y_masks[i][0], z_upper),
                (x_main[1], y_masks[i][1], z_lower),
            )
            for a in range(3):
                store(PF + a, p[a])
            for a in range(6):
                store(QF + a, q[a])
        return carry

    def primal_main(level, carry):
        z_upper, z_lower = z_main(level)
        for (i, row) in enumerate(starts):
            load, store, store_bar = main_refs(level, row)
            here = pl.ds(row, 8)
            p = [load(PF + a) for a in range(3)]
            q = [load(QF + a) for a in range(6)]
            prev_p = [
                jnp.where(first, from_low(side[PF, 0, here, :], level), pltpu.roll(p[0], 1, 1)),
                ext[PF + 1, level, pl.ds(row - 1, 8), :],
                ext[PF + 2, level - 1, here, :],
            ]
            next_q = [
                [
                    jnp.where(
                        last,
                        from_high(side[QF + j, 1, here, :], level),
                        pltpu.roll(q[j], LANES - 1, 1),
                    )
                    for j in ROWS_OF_Q[0]
                ],
                [ext[QF + j, level, pl.ds(row + 1, 8), :] for j in ROWS_OF_Q[1]],
                [ext[QF + j, level + 1, here, :] for j in ROWS_OF_Q[2]],
            ]
            new_u, new_v, bar = primal_step_of(
                load(U),
                [load(V + a) for a in range(3)],
                load(F),
                load(W),
                p,
                q,
                prev_p,
                next_q,
                (x_main[0], y_masks[i][0], z_upper),
                (x_main[1], y_masks[i][1], z_lower),
            )
            for a, value in enumerate([new_u] + new_v):
                store(U + a, value)
            for a in range(4):
                store_bar(a, bar[a])
        return carry

    def dual_side(which):
        updates = []
        for (i, row) in enumerate(starts):
            load, _, _ = side_refs(which, row)
            here = pl.ds(row, 8)
            bar = [side_bars[a, which, here, :] for a in range(4)]
            next_bar = [
                pltpu.roll(bar[0], LANES - 1, 1),
                side_bars[0, which, pl.ds(row + 1, 8), :],
                pltpu.roll(bar[0], LANES - SLOT, 1),
            ]
            prev_bar = [
                [pltpu.roll(bar[1 + a], 1, 1) for a in range(3)],
                [side_bars[1 + a, which, pl.ds(row - 1, 8), :] for a in range(3)],
                [pltpu.roll(bar[1 + a], SLOT, 1) for a in range(3)],
            ]
            p, q = dual_step_of(
                bar,
                next_bar,
                prev_bar,
                [load(PF + a) for a in range(3)],
                [load(QF + a) for a in range(6)],
                (x_side[which][0], y_masks[i][0], z_side[0]),
                (x_side[which][1], y_masks[i][1], z_side[1]),
            )
            for a, value in enumerate(p + q):
                side[PF + a, which, here, :] = value

    def primal_side(which):
        for (i, row) in enumerate(starts):
            load, store, store_bar = side_refs(which, row)
            here = pl.ds(row, 8)
            p = [load(PF + a) for a in range(3)]
            q = [load(QF + a) for a in range(6)]
            prev_p = [
                pltpu.roll(p[0], 1, 1),
                side[PF + 1, which, pl.ds(row - 1, 8), :],
                pltpu.roll(p[2], SLOT, 1),
            ]
            next_q = [
                [pltpu.roll(q[j], LANES - 1, 1) for j in ROWS_OF_Q[0]],
                [side[QF + j, which, pl.ds(row + 1, 8), :] for j in ROWS_OF_Q[1]],
                [pltpu.roll(q[j], LANES - SLOT, 1) for j in ROWS_OF_Q[2]],
            ]
            new_u, new_v, bar = primal_step_of(
                load(U),
                [load(V + a) for a in range(3)],
                load(F),
                load(W),
                p,
                q,
                prev_p,
                next_q,
                (x_side[which][0], y_masks[i][0], z_side[0]),
                (x_side[which][1], y_masks[i][1], z_side[1]),
            )
            for a, value in enumerate([new_u] + new_v):
                store(U + a, value)
            for a in range(4):
                store_bar(a, bar[a])

    def out_copies(fields):
        own = (pl.ds(HALO, nz), pl.ds(ROW0, ny))
        return [
            pltpu.make_async_copy(ext.at[(field,) + own], out, sem) for field, out in fields
        ]

    duals = [(pl.ds(PF, 3), out_p), (pl.ds(QF, 6), out_q)]
    primals = [(U, out_u), (pl.ds(V, 3), out_v)]

    def iteration(step, carry):
        paired_loop(step, levels - step, dual_main)
        for which in (0, 1):
            dual_side(which)

        @pl.when(step == ITERS - 1)
        def _():
            for copy in out_copies(duals):
                copy.start()

        paired_loop(step + 1, levels - 1 - step, primal_main)
        for which in (0, 1):
            primal_side(which)
        return carry

    lax.fori_loop(0, ITERS, iteration, 0)
    for copy in out_copies(primals):
        copy.start()
    for copy in out_copies(duals + primals):
        copy.wait()


def per_device(sizes, noisy_image, fidelity, primal_u, primal_v, dual_p, dual_q):
    nz, ny, nx = extents = noisy_image.shape
    levels, rows = nz + 2 * HALO, ny + 2 * ROW0
    assert nx == LANES and ny % 8 == 0 and levels * SLOT <= LANES
    assert min(nz, ny) >= HALO
    xs, ys, zs = (colours(sizes[axis]) for axis in AXES)
    combos = list(itertools.product(zs, ys))
    pos = jnp.stack([lax.axis_index(axis) for axis in AXES])
    args = tuple(pltpu.with_memory_space_constraint(a, pltpu.HBM) for a in (noisy_image, fidelity, primal_u, primal_v, dual_p, dual_q))
    f32 = jnp.float32
    smem = pl.BlockSpec(memory_space=pltpu.SMEM)
    anywhere = pl.BlockSpec(memory_space=pltpu.HBM)
    vmem = pl.BlockSpec(memory_space=pltpu.VMEM)

    def shaped(*shape):
        return jax.ShapeDtypeStruct(shape, f32)

    def call(body, ins, outs, out_specs, name, limit, **more):
        return pl.pallas_call(
            body,
            in_specs=ins,
            out_specs=out_specs,
            out_shape=outs,
            name=name,
            compiler_params=pltpu.CompilerParams(vmem_limit_bytes=limit * 1024 * 1024),
            **more,
        )

    z_pay = call(
        functools.partial(pack_z, extents, zs),
        [smem] + [anywhere] * 6,
        [shaped(SENT, ny, nx)] * len(zs),
        [vmem] * len(zs),
        "pack_z",
        8,
        scratch_shapes=[pltpu.SemaphoreType.DMA],
    )(pos, *args)
    z_got = [exchange(pay, {"gz": c}, sizes) for c, pay in zip(zs, z_pay)]

    strip_rows = 8 * len(tile_starts(ny))
    ext_shape = shaped(FIELDS, levels, rows, nx)
    own = call(
        functools.partial(pack_own, extents, ys, zs),
        [smem] + [anywhere] * 6,
        [ext_shape]
        + [shaped(SENT, nz, nx)] * len(ys)
        + [shaped(SENT * HALO, nx)] * len(combos),
        [vmem] * (1 + len(ys) + len(combos)),
        "pack_own",
        16,
        scratch_shapes=[pltpu.SemaphoreType.DMA],
    )(pos, *args)
    ext, y_pay, yz_pay = own[0], own[1 : 1 + len(ys)], own[1 + len(ys) :]
    yz_got = [exchange(pay, {"gz": a, "gy": b}, sizes) for (a, b), pay in zip(combos, yz_pay)]
    y_got = [exchange(pay, {"gy": c}, sizes) for c, pay in zip(ys, y_pay)]

    joined = call(
        functools.partial(join_halo, extents, xs, ys, zs),
        [smem] + [vmem] * (1 + len(zs) + len(ys) + len(combos)),
        [ext_shape, shaped(FIELDS, rows, nx)] + [shaped(GROUPS, strip_rows, nx)] * len(xs),
        [vmem] * (2 + len(xs)),
        "join_halo",
        20,
        input_output_aliases={1: 0},
    )(pos, ext, *z_got, *y_got, *yz_got)
    ext, strip, x_pay = joined[0], joined[1], joined[2:]
    x_got = [exchange(pay, {"gx": c}, sizes) for c, pay in zip(xs, x_pay)]

    solved = call(
        functools.partial(solve, extents, sizes, xs),
        [smem] + [vmem] * (2 + len(xs)),
        [ext_shape] + [shaped(*a.shape) for a in (primal_u, primal_v, dual_p, dual_q)],
        [vmem] + [anywhere] * 4,
        "solve",
        24,
        input_output_aliases={1: 0},
        scratch_shapes=[
            pltpu.VMEM((FIELDS, 2, rows, nx), f32),
            pltpu.VMEM((4, levels + 2, rows, nx), f32),
            pltpu.VMEM((4, 2, rows, nx), f32),
            pltpu.SemaphoreType.DMA,
        ],
    )(pos, ext, strip, *x_got)
    return tuple(solved[1:])


def solution(mesh):
    sizes = {axis: mesh.shape[axis] for axis in AXES}
    scalar, stacked = P("gz", "gy", "gx"), P(None, "gz", "gy", "gx")
    return jax.shard_map(
        functools.partial(per_device, sizes),
        mesh=mesh,
        in_specs=(scalar,) * 3 + (stacked,) * 3,
        out_specs=(scalar,) + (stacked,) * 3,
        check_vma=False,
    )
```

```python
import functools
import itertools

import jax
import jax.numpy as jnp
from jax import lax
from jax.experimental import pallas as pl
from jax.experimental.pallas import tpu as pltpu
from jax.sharding import PartitionSpec as P


ITERS = 3
HALO = ITERS
ROW0 = 8
SLOT = 8
LANES = 128

first_alpha = 0.5
second_alpha = 1.0
dual_step = 0.2
primal_step = 0.2

AXES = ("gx", "gy", "gz")
FIELDS = 15
F, W, U, V, PF, QF = 0, 1, 2, 3, 6, 9
GROUPS = (FIELDS + 1) // 2


def spans(low):
    chosen = [(F, 2), (W, 2), (U, 3), (V, 3), (V + 1, 3), (V + 2, 3)]
    chosen += [(PF + i, 2 if low else 3) for i in range(3)]
    chosen += [(QF + i, 3 if low else 2) for i in range(6)]
    if not low:
        chosen += [(U, 3)]
    return [(field, 0 if low else -count, count) for field, count in chosen]


def entries(low):
    return [(field, first + i) for field, first, count in spans(low) for i in range(count)]


SENT = len(entries(True))


def colours(size):
    return ("even", "odd")[: min(size - 1, 2)]


def partner(place, colour, size):
    other = place ^ 1 if colour == "even" else ((place + 1) ^ 1) - 1
    return other if 0 <= other < size else None


def exchange(values, moves, sizes):
    pairs = []
    for place in itertools.product(*(range(sizes[axis]) for axis in AXES)):
        other = list(place)
        for axis, colour in moves.items():
            other[AXES.index(axis)] = partner(place[AXES.index(axis)], colour, sizes[axis])
        if None in other:
            spare = [axis for axis in AXES if axis not in moves and sizes[axis] % 2 == 0]
            if not spare:
                continue
            other = list(place)
            other[AXES.index(spare[0])] ^= 1
        source, target = 0, 0
        for axis, here, there in zip(AXES, place, other):
            source = source * sizes[axis] + here
            target = target * sizes[axis] + there
        pairs.append((source, target))
    return lax.ppermute(values, AXES, pairs)


def sends_low(colour, parity):
    return (colour == "even") == (parity == 1)


def colour_of(side, parity):
    return "even" if (side == "low") == (parity == 1) else "odd"


def pick(received, colour):
    return received.get(colour, received["even"])


def pack(extents, ys, zs, pos, f, w, u, v, p, q, ext, *rest):
    nz, ny, _ = extents
    rows = ny + 2 * ROW0
    y_outs = dict(zip(ys, rest))
    z_outs = dict(zip(zs, rest[len(ys) :]))
    own_sem, z_sem = rest[-2:]
    arrays = ((F, f, 1), (W, w, 1), (U, u, 1), (V, v, 3), (PF, p, 3), (QF, q, 6))
    own = (pl.ds(HALO, nz), pl.ds(ROW0, ny))
    copies = []
    for base, array, count in arrays:
        fields = base if count == 1 else pl.ds(base, count)
        copies.append(pltpu.make_async_copy(array, ext.at[(fields,) + own], own_sem))
    for copy in copies:
        copy.start()

    def source(field, first, count):
        layers = pl.ds(first % nz, count)
        base, array, stack = [item for item in arrays if item[0] <= field][-1]
        return array.at[layers] if stack == 1 else array.at[field - base, layers]

    def z_copies(parity):
        for colour, out in z_outs.items():
            at = 0
            for field, first, count in spans(sends_low(colour, parity)):
                target = out.at[pl.ds(at, count)]
                yield pltpu.make_async_copy(source(field, first, count), target, z_sem)
                at += count

    for parity in (0, 1):

        @pl.when(pos[2] % 2 == parity)
        def _():
            for copy in z_copies(parity):
                copy.start()

    for copy in copies:
        copy.wait()
    flat = ext.reshape(FIELDS * (nz + 2 * HALO) * rows, LANES)
    for parity in (0, 1):

        @pl.when(pos[1] % 2 == parity)
        def _():
            for colour, out in y_outs.items():
                for i, (field, at) in enumerate(entries(sends_low(colour, parity))):
                    start = (field * (nz + 2 * HALO) + HALO) * rows + ROW0 + at % ny
                    out[i] = flat[pl.ds(start, nz, stride=rows), :]

    for copy in z_copies(0):
        copy.wait()


def tile_starts(ny):
    return [ROW0 - HALO + 8 * i for i in range(-(-(ny + 2 * HALO) // 8))]


def lanes_of():
    lane = lax.broadcasted_iota(jnp.int32, (8, LANES), 1)
    return lane, lane % SLOT


def placed(side, extent):
    if side == "low":
        return entries(False)[: SENT - HALO]
    return [(field, extent + at) for field, at in entries(True)]


def columns_of(values, level, shift=0):
    return pltpu.roll(values, (level * SLOT + HALO + shift) % LANES, 1)


def join_y(extents, ys, pos, ext_in, *rest):
    del ext_in
    nz, ny, _ = extents
    rows = ny + 2 * ROW0
    levels = nz + 2 * HALO
    y_got = dict(zip(ys, rest))
    ext, payload = rest[len(ys) :]
    flat = ext.reshape(FIELDS * levels * rows, LANES)
    for parity in (0, 1):

        @pl.when(pos[1] % 2 == parity)
        def _():
            for side in ("low", "high"):
                got = pick(y_got, colour_of(side, parity))
                for i, (field, at) in enumerate(placed(side, ny)):
                    start = (field * levels + HALO) * rows + ROW0 + at
                    flat[pl.ds(start, nz, stride=rows), :] = got[i]

    lane, _ = lanes_of()
    pieces = []
    for half, level in itertools.product((0, 1), range(HALO, HALO + nz)):
        shift = half * (LANES // 2)
        pieces.append(((level * SLOT + shift) % LANES, half, level, shift))
    pieces.sort()

    def group(i, carry):
        pair = (2 * i, jnp.minimum(2 * i + 1, FIELDS - 1))
        totals = []
        for row in tile_starts(ny):
            total = None
            for at, half, level, shift in pieces:
                turned = columns_of(ext[pair[half], level, pl.ds(row, 8), :], level, shift)
                total = turned if total is None else jnp.where(lane >= at, turned, total)
            totals.append(total)
        for j, total in enumerate(totals):
            payload[i, pl.ds(8 * j, 8), :] = total
        return carry

    lax.fori_loop(0, GROUPS, group, 0)


BLOCK = HALO * SLOT
PER_TILE = LANES // BLOCK
BLOCKS = -(-FIELDS // PER_TILE)


def join_x(extents, xs, ys, zs, pos, ext, payload, *rest):
    nz, ny, _ = extents
    x_got = dict(zip(xs, rest))
    side = rest[len(xs)]
    z_outs = dict(zip(zs, rest[len(xs) + 1 :]))
    lane, slot = lanes_of()
    starts = tile_starts(ny)
    half = LANES // 2

    def build(got_low, got_high, outs):
        def group(i, carry):
            sides = []
            for j in range(len(starts)):
                at = pl.ds(8 * j, 8)
                own = payload[i, at, :]
                left = jnp.where(slot < HALO, got_low[i, at, :], own)
                right = jnp.where(slot < HALO, own, got_high[i, at, :])
                sides.append((left, right, pltpu.roll(left, half, 1), pltpu.roll(right, half, 1)))
            for values, row in zip(sides, starts):
                for k in range(4):
                    side[2 * i + k // 2, k % 2, pl.ds(row, 8), :] = values[k]
            return carry

        lax.fori_loop(0, GROUPS, group, 0)

        def border(j, carry):
            at = pl.ds(pl.multiple_of(8 * j, 8), 8)
            came = [
                jnp.where(slot < HALO, got_low[i, at, :], got_high[i, at, :]) for i in range(GROUPS)
            ]
            made = []
            for low, out in outs.items():
                for block in range(BLOCKS):
                    total = None
                    for k in range(min(PER_TILE, FIELDS - block * PER_TILE)):
                        i, odd = divmod(block * PER_TILE + k, 2)
                        first = HALO * SLOT if low else nz * SLOT
                        turned = pltpu.roll(came[i], (odd * half + k * BLOCK - first) % LANES, 1)
                        total = turned if total is None else jnp.where(lane >= k * BLOCK, turned, total)
                    made.append((out, block, total))
            for out, block, total in made:
                here = pl.ds(pl.multiple_of(8 * (block * len(starts) + j), 8), 8)
                out[here, :] = total
            return carry

        lax.fori_loop(0, len(starts), border, 0)

    for x_parity, z_parity in itertools.product((0, 1), (0, 1)):

        @pl.when(jnp.logical_and(pos[0] % 2 == x_parity, pos[2] % 2 == z_parity))
        def _():
            build(
                pick(x_got, colour_of("low", x_parity)),
                pick(x_got, colour_of("high", x_parity)),
                {sends_low(colour, z_parity): out for colour, out in z_outs.items()},
            )

    for z_parity, y_parity in itertools.product((0, 1), (0, 1)):

        @pl.when(jnp.logical_and(pos[2] % 2 == z_parity, pos[1] % 2 == y_parity))
        def _():
            for z_colour, out in z_outs.items():
                for n, y_colour in enumerate(ys):
                    low = colour_of("low", y_parity) == y_colour
                    row = ROW0 - HALO if low else ROW0 + ny
                    first = BLOCKS * 8 * len(starts) + n * SENT * HALO
                    for i, (field, at) in enumerate(entries(sends_low(z_colour, z_parity))):
                        out[pl.ds(first + i * HALO, HALO), :] = ext[
                            field, HALO + at % nz, pl.ds(row, HALO), :
                        ]


def shrink(total, bound):
    return lax.rsqrt(jnp.maximum(1.0, total * (1.0 / (bound * bound))))


def masked(mask, values):
    return values if mask is None else mask * values


def p_step(bar, next_bar, p, upper):
    t = [p[a] + masked(upper[a], next_bar[a] - bar[0]) - bar[1 + a] for a in range(3)]
    scale = shrink(t[0] * t[0] + t[1] * t[1] + t[2] * t[2], first_alpha)
    return [value * scale for value in t]


def q_step(bar, prev_bar, q, lower):
    d = [[masked(lower[b], bar[a] - prev_bar[b][a]) for a in range(3)] for b in range(3)]
    s = [q[a] + d[a][a] for a in range(3)]
    for i, (a, b) in enumerate(((0, 1), (0, 2), (1, 2))):
        s.append(q[3 + i] + 0.5 * (d[b][a] + d[a][b]))
    off = s[3] * s[3] + s[4] * s[4] + s[5] * s[5]
    scale = shrink(s[0] * s[0] + s[1] * s[1] + s[2] * s[2] + (off + off), second_alpha)
    return [value * scale for value in s]


ROWS_OF_Q = ((0, 3, 4), (3, 1, 5), (4, 5, 2))


def primal_step_of(u, v, a_map, b_map, p, q, prev_p, next_q, upper, lower):
    div = None
    for a in range(3):
        term = masked(upper[a], p[a]) - masked(lower[a], prev_p[a])
        div = term if div is None else div + term
    new_u = (u + primal_step * div) * b_map + a_map
    new_v = []
    for a in range(3):
        total = p[a]
        for b in range(3):
            total = total + (masked(upper[b], next_q[b][a]) - masked(lower[b], q[ROWS_OF_Q[b][a]]))
        new_v.append(v[a] + primal_step * total)
    bar = [(2.0 * dual_step) * new_u - dual_step * u]
    bar += [(2.0 * dual_step) * new_v[a] - dual_step * v[a] for a in range(3)]
    return new_u, new_v, bar


class Steps:
    def __init__(self, extents, sizes, pos, ext, bars, side, side_bars):
        self.nz, self.ny, self.nx = nz, ny, nx = extents
        self.levels = nz + 2 * HALO
        self.pos, self.ext, self.bars, self.side, self.side_bars = pos, ext, bars, side, side_bars
        self.starts = tile_starts(ny)
        self.lane, slot = lanes_of()
        sub = lax.broadcasted_iota(jnp.int32, (8, LANES), 0)
        self.full = full = [sizes[axis] * extent for axis, extent in zip(AXES, (nx, ny, nz))]

        def masks(places, extent):
            upper = jnp.logical_and(places >= 0, places < extent - 1)
            lower = jnp.logical_and(places > 0, places < extent)
            return upper.astype(jnp.float32), lower.astype(jnp.float32)

        outer = (self.starts[0], self.starts[-1])
        self.y_masks = [
            masks(pos[1] * ny + (row - ROW0) + sub, full[1]) if row in outer else (None, None)
            for row in self.starts
        ]
        self.x_main = masks(pos[0] * nx + self.lane, full[0])
        self.x_side = [masks(pos[0] * nx + at + slot, full[0]) for at in (-HALO, nx - HALO)]
        self.z_side = masks(pos[2] * nz - HALO + self.lane // SLOT, full[2])
        self.first, self.last = self.lane == 0, self.lane == LANES - 1

    def z_main(self, level):
        place = self.pos[2] * self.nz - HALO + level
        upper = jnp.logical_and(place >= 0, place < self.full[2] - 1)
        lower = jnp.logical_and(place > 0, place < self.full[2])
        one, none = jnp.float32(1.0), jnp.float32(0.0)
        return jnp.where(upper, one, none), jnp.where(lower, one, none)

    def from_low(self, values, level):
        return pltpu.roll(values, LANES - HALO + 1 - SLOT * level, 1)

    def from_high(self, values, level):
        return pltpu.roll(values, LANES - 1 - HALO - SLOT * level, 1)

    def next_x(self, values, field_values, level):
        return jnp.where(self.last, self.from_high(field_values, level), pltpu.roll(values, LANES - 1, 1))

    def prev_x(self, values, field_values, level):
        return jnp.where(self.first, self.from_low(field_values, level), pltpu.roll(values, 1, 1))

    @staticmethod
    def maps(f, w):
        inverse = 1.0 / (1.0 + primal_step * w)
        return (primal_step * w * f) * inverse, inverse

    def prepare_main(self, level):
        for row in self.starts:
            here = pl.ds(row, 8)
            maps = self.maps(self.ext[F, level, here, :], self.ext[W, level, here, :])
            self.ext[F, level, here, :], self.ext[W, level, here, :] = maps
            for a in range(4):
                self.bars[a, level + 1, here, :] = dual_step * self.ext[U + a, level, here, :]

    def prepare_side(self, which, row, fields):
        here = pl.ds(row, 8)
        for field, values in enumerate(list(self.maps(fields[F], fields[W])) + fields[U:]):
            self.side[field, which, here, :] = values
        for a in range(4):
            self.side_bars[a, which, here, :] = dual_step * fields[U + a]

    def p_main(self, level):
        ext, bars = self.ext, self.bars
        upper_z, _ = self.z_main(level)
        for i, row in enumerate(self.starts):
            here = pl.ds(row, 8)
            bar = [bars[a, level + 1, here, :] for a in range(4)]
            next_bar = [
                self.next_x(bar[0], self.side_bars[0, 1, here, :], level),
                bars[0, level + 1, pl.ds(row + 1, 8), :],
                bars[0, level + 2, here, :],
            ]
            p = [ext[PF + a, level, here, :] for a in range(3)]
            p = p_step(bar, next_bar, p, (self.x_main[0], self.y_masks[i][0], upper_z))
            for a in range(3):
                ext[PF + a, level, here, :] = p[a]

    def q_main(self, level):
        ext, bars = self.ext, self.bars
        _, lower_z = self.z_main(level)
        for i, row in enumerate(self.starts):
            here = pl.ds(row, 8)
            bar = [bars[1 + a, level + 1, here, :] for a in range(3)]
            prev_bar = [
                [self.prev_x(bar[a], self.side_bars[1 + a, 0, here, :], level) for a in range(3)],
                [bars[1 + a, level + 1, pl.ds(row - 1, 8), :] for a in range(3)],
                [bars[1 + a, level, here, :] for a in range(3)],
            ]
            q = [ext[QF + a, level, here, :] for a in range(6)]
            q = q_step(bar, prev_bar, q, (self.x_main[1], self.y_masks[i][1], lower_z))
            for a in range(6):
                ext[QF + a, level, here, :] = q[a]

    def primal_main(self, level):
        ext, bars, side = self.ext, self.bars, self.side
        upper_z, lower_z = self.z_main(level)
        for i, row in enumerate(self.starts):
            here = pl.ds(row, 8)
            p = [ext[PF + a, level, here, :] for a in range(3)]
            q = [ext[QF + a, level, here, :] for a in range(6)]
            prev_p = [
                self.prev_x(p[0], side[PF, 0, here, :], level),
                ext[PF + 1, level, pl.ds(row - 1, 8), :],
                ext[PF + 2, level - 1, here, :],
            ]
            next_q = [
                [self.next_x(q[j], side[QF + j, 1, here, :], level) for j in ROWS_OF_Q[0]],
                [ext[QF + j, level, pl.ds(row + 1, 8), :] for j in ROWS_OF_Q[1]],
                [ext[QF + j, level + 1, here, :] for j in ROWS_OF_Q[2]],
            ]
            new_u, new_v, bar = primal_step_of(
                ext[U, level, here, :],
                [ext[V + a, level, here, :] for a in range(3)],
                ext[F, level, here, :],
                ext[W, level, here, :],
                p,
                q,
                prev_p,
                next_q,
                (self.x_main[0], self.y_masks[i][0], upper_z),
                (self.x_main[1], self.y_masks[i][1], lower_z),
            )
            for a, value in enumerate([new_u] + new_v):
                ext[U + a, level, here, :] = value
            for a in range(4):
                bars[a, level + 1, here, :] = bar[a]

    def dual_side(self):
        side, side_bars = self.side, self.side_bars
        for which, (i, row) in itertools.product((0, 1), enumerate(self.starts)):
            here = pl.ds(row, 8)
            bar = [side_bars[a, which, here, :] for a in range(4)]
            next_bar = [
                pltpu.roll(bar[0], LANES - 1, 1),
                side_bars[0, which, pl.ds(row + 1, 8), :],
                pltpu.roll(bar[0], LANES - SLOT, 1),
            ]
            prev_bar = [
                [pltpu.roll(bar[1 + a], 1, 1) for a in range(3)],
                [side_bars[1 + a, which, pl.ds(row - 1, 8), :] for a in range(3)],
                [pltpu.roll(bar[1 + a], SLOT, 1) for a in range(3)],
            ]
            upper = (self.x_side[which][0], self.y_masks[i][0], self.z_side[0])
            lower = (self.x_side[which][1], self.y_masks[i][1], self.z_side[1])
            p = p_step(bar, next_bar, [side[PF + a, which, here, :] for a in range(3)], upper)
            q = q_step(bar[1:], prev_bar, [side[QF + a, which, here, :] for a in range(6)], lower)
            for a, value in enumerate(p + q):
                side[PF + a, which, here, :] = value

    def primal_side(self):
        side, side_bars = self.side, self.side_bars
        for which, (i, row) in itertools.product((0, 1), enumerate(self.starts)):
            here = pl.ds(row, 8)
            p = [side[PF + a, which, here, :] for a in range(3)]
            q = [side[QF + a, which, here, :] for a in range(6)]
            prev_p = [
                pltpu.roll(p[0], 1, 1),
                side[PF + 1, which, pl.ds(row - 1, 8), :],
                pltpu.roll(p[2], SLOT, 1),
            ]
            next_q = [
                [pltpu.roll(q[j], LANES - 1, 1) for j in ROWS_OF_Q[0]],
                [side[QF + j, which, pl.ds(row + 1, 8), :] for j in ROWS_OF_Q[1]],
                [pltpu.roll(q[j], LANES - SLOT, 1) for j in ROWS_OF_Q[2]],
            ]
            new_u, new_v, bar = primal_step_of(
                side[U, which, here, :],
                [side[V + a, which, here, :] for a in range(3)],
                side[F, which, here, :],
                side[W, which, here, :],
                p,
                q,
                prev_p,
                next_q,
                (self.x_side[which][0], self.y_masks[i][0], self.z_side[0]),
                (self.x_side[which][1], self.y_masks[i][1], self.z_side[1]),
            )
            for a, value in enumerate([new_u] + new_v):
                side[U + a, which, here, :] = value
            for a in range(4):
                side_bars[a, which, here, :] = bar[a]


def level_loop(start, stop, *bodies):
    count = max(stop - start, 0)

    def trip(i, carry):
        for body in bodies:
            for j in (0, 1):
                body(start + 2 * i + j)
        return carry

    lax.fori_loop(0, count // 2, trip, 0)
    if count % 2:
        for body in bodies:
            body(stop - 1)


def solve_inner(extents, sizes, pos, ext_in, side_in, ext, bars, side, side_bars):
    del ext_in
    nz, _, _ = extents
    steps = Steps(extents, sizes, pos, ext, bars, side, side_bars)
    for which, row in itertools.product((0, 1), steps.starts):
        fields = [side_in[field, which, pl.ds(row, 8), :] for field in range(FIELDS)]
        steps.prepare_side(which, row, fields)
    level_loop(HALO, HALO + nz, steps.prepare_main)
    for step in range(ITERS):
        low, high = HALO + step, HALO + nz - step
        if high - 1 <= low:
            break
        level_loop(low, high - 1, steps.p_main, lambda level: steps.q_main(level + 1))
        if high - 2 < low + 1:
            break
        steps.dual_side()
        level_loop(low + 1, high - 1, steps.primal_main)
        if step + 1 < ITERS:
            steps.primal_side()


def solve_outer(extents, sizes, ys, zs, pos, ext_in, bars_in, side_in, *rest):
    del ext_in, bars_in
    nz, ny, _ = extents
    z_got = dict(zip(zs, rest))
    rest = rest[len(zs) :]
    frame_got = dict(zip(zs, rest))
    ext, bars, out_u, out_v, out_p, out_q, side, side_bars, sem = rest[len(zs) :]
    steps = Steps(extents, sizes, pos, ext, bars, side, side_bars)
    starts = steps.starts
    lane, slot = lanes_of()
    sides = ("low", "high")

    for z_parity in (0, 1):

        @pl.when(pos[2] % 2 == z_parity)
        def _():
            for z_side in sides:
                got = pick(z_got, colour_of(z_side, z_parity))
                for i, (field, at) in enumerate(placed(z_side, nz)):
                    ext[field, HALO + at, pl.ds(ROW0, ny), :] = got[i]

    for z_parity, y_parity in itertools.product((0, 1), (0, 1)):

        @pl.when(jnp.logical_and(pos[2] % 2 == z_parity, pos[1] % 2 == y_parity))
        def _():
            for z_side, y_side in itertools.product(sides, sides):
                got = pick(frame_got, colour_of(z_side, z_parity))
                y_colour = colour_of(y_side, y_parity)
                n = ys.index(y_colour) if y_colour in ys else 0
                first = BLOCKS * 8 * len(starts) + n * SENT * HALO
                row = ROW0 + (-HALO if y_side == "low" else ny)
                for i, (field, at) in enumerate(placed(z_side, nz)):
                    ext[field, HALO + at, pl.ds(row, HALO), :] = got[pl.ds(first + i * HALO, HALO), :]

    top = (HALO + nz) * SLOT
    below, above = lane < BLOCK, lane >= top
    low_levels, high_levels = range(HALO), range(HALO + nz, nz + 2 * HALO)

    outer = jnp.logical_or(below, above)

    def strips(got_low, got_high):
        ready = None
        for j, row in enumerate(starts):
            here = pl.ds(row, 8)
            fields = ([], [])
            for field in range(FIELDS):
                block, k = divmod(field, PER_TILE)
                columns = None
                for level in list(low_levels) + list(high_levels):
                    turned = columns_of(ext[field, level, here, :], level)
                    columns = turned if columns is None else jnp.where(lane >= level * SLOT, turned, columns)
                at = (pl.ds(8 * (block * len(starts) + j), 8), slice(None))
                came = jnp.where(
                    above,
                    pltpu.roll(got_high[at], (top - k * BLOCK) % LANES, 1),
                    pltpu.roll(got_low[at], (-k * BLOCK) % LANES, 1),
                )
                left = jnp.where(slot < HALO, came, columns)
                right = jnp.where(slot < HALO, columns, came)
                fields[0].append(jnp.where(outer, left, side_in[field, 0, here, :]))
                fields[1].append(jnp.where(outer, right, side_in[field, 1, here, :]))
            for done in (ready, (row, fields)):
                if done is not None and (done is ready or row == starts[-1]):
                    for which in (0, 1):
                        steps.prepare_side(which, done[0], done[1][which])
            ready = (row, fields)

    for z_parity in (0, 1):

        @pl.when(pos[2] % 2 == z_parity)
        def _():
            strips(
                pick(frame_got, colour_of("low", z_parity)),
                pick(frame_got, colour_of("high", z_parity)),
            )

    for level in list(low_levels) + list(high_levels):
        steps.prepare_main(level)

    def out_copies(fields):
        own = (pl.ds(HALO, nz), pl.ds(ROW0, ny))
        return [pltpu.make_async_copy(ext.at[(field,) + own], out, sem) for field, out in fields]

    duals = [(pl.ds(PF, 3), out_p), (pl.ds(QF, 6), out_q)]
    primals = [(U, out_u), (pl.ds(V, 3), out_v)]
    apart = nz >= 2 * ITERS

    def outer_levels(low_first, high_first):
        if apart:
            return [first + j for first in (low_first, high_first) for j in range(HALO)]
        return sorted({first + j for first in (low_first, high_first) for j in range(HALO)})

    def iteration(step, carry):
        top_level = HALO + nz - 1 - step
        for level in outer_levels(step, top_level):
            steps.p_main(level)
        for level in outer_levels(step + 1, top_level + 1):
            steps.q_main(level)

        @pl.when(step == ITERS - 1)
        def _():
            for copy in out_copies(duals):
                copy.start()

        steps.dual_side()
        for level in outer_levels(step + 1, top_level):
            steps.primal_main(level)
        pl.when(step < ITERS - 1)(steps.primal_side)
        return carry

    if apart:
        lax.fori_loop(0, ITERS, iteration, 0)
    else:
        for step in range(ITERS):
            iteration(step, 0)
    for copy in out_copies(primals):
        copy.start()
    for copy in out_copies(duals + primals):
        copy.wait()


def per_device(sizes, noisy_image, fidelity, primal_u, primal_v, dual_p, dual_q):
    nz, ny, nx = extents = noisy_image.shape
    levels, rows = nz + 2 * HALO, ny + 2 * ROW0
    assert nx == LANES and ny % 8 == 0 and nz * SLOT <= LANES // 2
    assert min(nz, ny) >= HALO and min(sizes.values()) > 1
    xs, ys, zs = (colours(sizes[axis]) for axis in AXES)
    pos = jnp.stack([lax.axis_index(axis) for axis in AXES])
    args = tuple(pltpu.with_memory_space_constraint(a, pltpu.HBM) for a in (noisy_image, fidelity, primal_u, primal_v, dual_p, dual_q))
    f32 = jnp.float32
    smem = pl.BlockSpec(memory_space=pltpu.SMEM)
    anywhere = pl.BlockSpec(memory_space=pltpu.HBM)
    vmem = pl.BlockSpec(memory_space=pltpu.VMEM)

    def shaped(*shape):
        return jax.ShapeDtypeStruct(shape, f32)

    def call(body, ins, outs, out_specs, limit, **more):
        return pl.pallas_call(
            body,
            in_specs=ins,
            out_specs=out_specs,
            out_shape=outs,
            compiler_params=pltpu.CompilerParams(vmem_limit_bytes=limit * 1024 * 1024),
            **more,
        )

    strip_rows = 8 * len(tile_starts(ny))
    ext_shape = shaped(FIELDS, levels, rows, nx)
    packed = call(
        functools.partial(pack, extents, ys, zs),
        [smem] + [anywhere] * 6,
        [ext_shape] + [shaped(SENT, nz, nx)] * len(ys) + [shaped(SENT, ny, nx)] * len(zs),
        [vmem] * (1 + len(ys) + len(zs)),
        16,
        scratch_shapes=[pltpu.SemaphoreType.DMA, pltpu.SemaphoreType.DMA],
    )(pos, *args)
    ext, y_pay, z_pay = packed[0], packed[1 : 1 + len(ys)], packed[1 + len(ys) :]
    y_got = [exchange(pay, {"gy": c}, sizes) for c, pay in zip(ys, y_pay)]
    z_got = [exchange(pay, {"gz": c}, sizes) for c, pay in zip(zs, z_pay)]

    ext, x_pay = call(
        functools.partial(join_y, extents, ys),
        [smem] + [vmem] * (1 + len(ys)),
        [ext_shape, shaped(GROUPS, strip_rows, nx)],
        [vmem] * 2,
        16,
        input_output_aliases={1: 0},
    )(pos, ext, *y_got)
    x_got = [exchange(x_pay, {"gx": c}, sizes) for c in xs]

    both = shaped(FIELDS, 2, rows, nx)
    frame = shaped(BLOCKS * strip_rows + len(ys) * SENT * HALO, nx)
    side, *frame_pay = call(
        functools.partial(join_x, extents, xs, ys, zs),
        [smem] + [vmem] * (2 + len(xs)),
        [shaped(2 * GROUPS, 2, rows, nx)] + [frame] * len(zs),
        [vmem] * (1 + len(zs)),
        16,
    )(pos, ext, x_pay, *x_got)
    frame_got = [exchange(pay, {"gz": c}, sizes) for c, pay in zip(zs, frame_pay)]

    bar_shape = shaped(4, levels + 2, rows, nx)
    scratch = [pltpu.VMEM(both.shape, f32), pltpu.VMEM((4,) + both.shape[1:], f32)]
    ext, bars = call(
        functools.partial(solve_inner, extents, sizes),
        [smem] + [vmem] * 2,
        [ext_shape, bar_shape],
        [vmem] * 2,
        16,
        input_output_aliases={1: 0},
        scratch_shapes=scratch,
    )(pos, ext, side)

    solved = call(
        functools.partial(solve_outer, extents, sizes, ys, zs),
        [smem] + [vmem] * (3 + 2 * len(zs)),
        [ext_shape, bar_shape] + [shaped(*a.shape) for a in (primal_u, primal_v, dual_p, dual_q)],
        [vmem] * 2 + [anywhere] * 4,
        24,
        input_output_aliases={1: 0, 2: 1},
        scratch_shapes=scratch + [pltpu.SemaphoreType.DMA],
    )(pos, ext, bars, side, *z_got, *frame_got)
    return tuple(solved[2:])


def solution(mesh):
    sizes = {axis: mesh.shape[axis] for axis in AXES}
    scalar, stacked = P("gz", "gy", "gx"), P(None, "gz", "gy", "gx")

    def body(*args):
        return per_device(sizes, *args)

    return jax.shard_map(
        body,
        mesh=mesh,
        in_specs=(scalar,) * 3 + (stacked,) * 3,
        out_specs=(scalar,) + (stacked,) * 3,
        check_vma=False,
    )
```

```python
import functools
import itertools

import jax
import jax.numpy as jnp
from jax import lax
from jax.experimental import pallas as pl
from jax.experimental.pallas import tpu as pltpu
from jax.sharding import PartitionSpec as P


ITERS = 3
HALO = ITERS
ROW0 = 8
SLOT = 8
LANES = 128

first_alpha = 0.5
second_alpha = 1.0
dual_step = 0.2
primal_step = 0.2

AXES = ("gx", "gy", "gz")
FIELDS = 15
F, W, U, V, PF, QF = 0, 1, 2, 3, 6, 9
GROUPS = (FIELDS + 1) // 2


def spans(low):
    chosen = [(F, 2), (W, 2), (U, 3), (V, 3), (V + 1, 3), (V + 2, 3)]
    chosen += [(PF + i, 2 if low else 3) for i in range(3)]
    chosen += [(QF + i, 3 if low else 2) for i in range(6)]
    if not low:
        chosen += [(U, 3)]
    return [(field, 0 if low else -count, count) for field, count in chosen]


def entries(low):
    return [(field, first + i) for field, first, count in spans(low) for i in range(count)]


SENT = len(entries(True))


def colours(size):
    return ("even", "odd")[: min(size - 1, 2)]


def partner(place, colour, size):
    other = place ^ 1 if colour == "even" else ((place + 1) ^ 1) - 1
    return other if 0 <= other < size else None


def exchange(values, moves, sizes):
    pairs = []
    for place in itertools.product(*(range(sizes[axis]) for axis in AXES)):
        other = list(place)
        for axis, colour in moves.items():
            other[AXES.index(axis)] = partner(place[AXES.index(axis)], colour, sizes[axis])
        if None in other:
            spare = [axis for axis in AXES if axis not in moves and sizes[axis] % 2 == 0]
            if not spare:
                continue
            other = list(place)
            other[AXES.index(spare[0])] ^= 1
        source, target = 0, 0
        for axis, here, there in zip(AXES, place, other):
            source = source * sizes[axis] + here
            target = target * sizes[axis] + there
        pairs.append((source, target))
    return lax.ppermute(values, AXES, pairs)


def sends_low(colour, parity):
    return (colour == "even") == (parity == 1)


def colour_of(side, parity):
    return "even" if (side == "low") == (parity == 1) else "odd"


def pick(received, colour):
    return received.get(colour, received["even"])


def pack(extents, ys, zs, f, w, u, v, p, q, ext, *rest):
    pos = place_of()
    nz, ny, _ = extents
    rows = ny + 2 * ROW0
    y_outs = dict(zip(ys, rest))
    z_outs = dict(zip(zs, rest[len(ys) :]))
    own_sem, z_sem = rest[-2:]
    arrays = ((F, f, 1), (W, w, 1), (U, u, 1), (V, v, 3), (PF, p, 3), (QF, q, 6))
    own = (pl.ds(HALO, nz), pl.ds(ROW0, ny))
    copies = []
    for base, array, count in arrays:
        fields = base if count == 1 else pl.ds(base, count)
        copies.append(pltpu.make_async_copy(array, ext.at[(fields,) + own], own_sem))
    for copy in copies:
        copy.start()

    def source(field, first, count):
        layers = pl.ds(first % nz, count)
        base, array, stack = [item for item in arrays if item[0] <= field][-1]
        return array.at[layers] if stack == 1 else array.at[field - base, layers]

    def z_copies(parity):
        for colour, out in z_outs.items():
            at = 0
            for field, first, count in spans(sends_low(colour, parity)):
                target = out.at[pl.ds(at, count)]
                yield pltpu.make_async_copy(source(field, first, count), target, z_sem)
                at += count

    for parity in (0, 1):

        @pl.when(pos[2] % 2 == parity)
        def _():
            for copy in z_copies(parity):
                copy.start()

    for copy in copies:
        copy.wait()
    flat = ext.reshape(FIELDS * (nz + 2 * HALO) * rows, LANES)
    for parity in (0, 1):

        @pl.when(pos[1] % 2 == parity)
        def _():
            for colour, out in y_outs.items():
                for i, (field, at) in enumerate(entries(sends_low(colour, parity))):
                    start = (field * (nz + 2 * HALO) + HALO) * rows + ROW0 + at % ny
                    out[i] = flat[pl.ds(start, nz, stride=rows), :]

    for copy in z_copies(0):
        copy.wait()


def tile_starts(ny):
    return [ROW0 - HALO + 8 * i for i in range(-(-(ny + 2 * HALO) // 8))]


def place_of():
    return [lax.axis_index(axis) for axis in AXES]


def lanes_of():
    lane = lax.broadcasted_iota(jnp.int32, (8, LANES), 1)
    return lane, lane % SLOT


def placed(side, extent):
    if side == "low":
        return entries(False)[: SENT - HALO]
    return [(field, extent + at) for field, at in entries(True)]


def columns_of(values, level, shift=0):
    return pltpu.roll(values, (level * SLOT + HALO + shift) % LANES, 1)


def join_y(extents, ys, ext_in, *rest):
    pos = place_of()
    del ext_in
    nz, ny, _ = extents
    rows = ny + 2 * ROW0
    levels = nz + 2 * HALO
    y_got = dict(zip(ys, rest))
    ext, payload = rest[len(ys) :]
    flat = ext.reshape(FIELDS * levels * rows, LANES)
    for parity in (0, 1):

        @pl.when(pos[1] % 2 == parity)
        def _():
            for side in ("low", "high"):
                got = pick(y_got, colour_of(side, parity))
                for i, (field, at) in enumerate(placed(side, ny)):
                    start = (field * levels + HALO) * rows + ROW0 + at
                    flat[pl.ds(start, nz, stride=rows), :] = got[i]

    lane, _ = lanes_of()
    pieces = []
    for half, level in itertools.product((0, 1), range(HALO, HALO + nz)):
        shift = half * (LANES // 2)
        pieces.append(((level * SLOT + shift) % LANES, half, level, shift))
    pieces.sort()

    def group(i, carry):
        pair = (2 * i, jnp.minimum(2 * i + 1, FIELDS - 1))
        totals = []
        for row in tile_starts(ny):
            total = None
            for at, half, level, shift in pieces:
                turned = columns_of(ext[pair[half], level, pl.ds(row, 8), :], level, shift)
                total = turned if total is None else jnp.where(lane >= at, turned, total)
            totals.append(total)
        for j, total in enumerate(totals):
            payload[i, pl.ds(8 * j, 8), :] = total
        return carry

    lax.fori_loop(0, GROUPS, group, 0)


BLOCK = HALO * SLOT
PER_TILE = LANES // BLOCK
BLOCKS = -(-FIELDS // PER_TILE)


def join_x(extents, xs, ys, zs, ext, payload, *rest):
    pos = place_of()
    nz, ny, _ = extents
    x_got = dict(zip(xs, rest))
    side = rest[len(xs)]
    z_outs = dict(zip(zs, rest[len(xs) + 1 :]))
    lane, slot = lanes_of()
    starts = tile_starts(ny)
    half = LANES // 2

    def build(got_low, got_high, outs):
        def group(i, carry):
            sides = []
            for j in range(len(starts)):
                at = pl.ds(8 * j, 8)
                own = payload[i, at, :]
                left = jnp.where(slot < HALO, got_low[i, at, :], own)
                right = jnp.where(slot < HALO, own, got_high[i, at, :])
                sides.append((left, right, pltpu.roll(left, half, 1), pltpu.roll(right, half, 1)))
            for values, row in zip(sides, starts):
                for k in range(4):
                    side[2 * i + k // 2, k % 2, pl.ds(row, 8), :] = values[k]
            return carry

        lax.fori_loop(0, GROUPS, group, 0)

        def border(j, carry):
            at = pl.ds(pl.multiple_of(8 * j, 8), 8)
            came = [
                jnp.where(slot < HALO, got_low[i, at, :], got_high[i, at, :]) for i in range(GROUPS)
            ]
            made = []
            for low, out in outs.items():
                for block in range(BLOCKS):
                    total = None
                    for k in range(min(PER_TILE, FIELDS - block * PER_TILE)):
                        i, odd = divmod(block * PER_TILE + k, 2)
                        first = HALO * SLOT if low else nz * SLOT
                        turned = pltpu.roll(came[i], (odd * half + k * BLOCK - first) % LANES, 1)
                        total = turned if total is None else jnp.where(lane >= k * BLOCK, turned, total)
                    made.append((out, block, total))
            for out, block, total in made:
                here = pl.ds(pl.multiple_of(8 * (block * len(starts) + j), 8), 8)
                out[here, :] = total
            return carry

        lax.fori_loop(0, len(starts), border, 0)

    for x_parity, z_parity in itertools.product((0, 1), (0, 1)):

        @pl.when(jnp.logical_and(pos[0] % 2 == x_parity, pos[2] % 2 == z_parity))
        def _():
            build(
                pick(x_got, colour_of("low", x_parity)),
                pick(x_got, colour_of("high", x_parity)),
                {sends_low(colour, z_parity): out for colour, out in z_outs.items()},
            )

    for z_parity, y_parity in itertools.product((0, 1), (0, 1)):

        @pl.when(jnp.logical_and(pos[2] % 2 == z_parity, pos[1] % 2 == y_parity))
        def _():
            for z_colour, out in z_outs.items():
                for n, y_colour in enumerate(ys):
                    low = colour_of("low", y_parity) == y_colour
                    row = ROW0 - HALO if low else ROW0 + ny
                    first = BLOCKS * 8 * len(starts) + n * SENT * HALO
                    for i, (field, at) in enumerate(entries(sends_low(z_colour, z_parity))):
                        out[pl.ds(first + i * HALO, HALO), :] = ext[
                            field, HALO + at % nz, pl.ds(row, HALO), :
                        ]


def shrink(total, bound):
    return lax.rsqrt(jnp.maximum(1.0, total * (1.0 / (bound * bound))))


def masked(mask, values):
    return values if mask is None else mask * values


def p_step(bar, next_bar, p, upper):
    t = [p[a] + masked(upper[a], next_bar[a] - bar[0]) - bar[1 + a] for a in range(3)]
    scale = shrink(t[0] * t[0] + t[1] * t[1] + t[2] * t[2], first_alpha)
    return [value * scale for value in t]


def q_step(bar, prev_bar, q, lower):
    d = [[masked(lower[b], bar[a] - prev_bar[b][a]) for a in range(3)] for b in range(3)]
    s = [q[a] + d[a][a] for a in range(3)]
    for i, (a, b) in enumerate(((0, 1), (0, 2), (1, 2))):
        s.append(q[3 + i] + 0.5 * (d[b][a] + d[a][b]))
    off = s[3] * s[3] + s[4] * s[4] + s[5] * s[5]
    scale = shrink(s[0] * s[0] + s[1] * s[1] + s[2] * s[2] + (off + off), second_alpha)
    return [value * scale for value in s]


ROWS_OF_Q = ((0, 3, 4), (3, 1, 5), (4, 5, 2))


def primal_step_of(u, v, a_map, b_map, p, q, prev_p, next_q, upper, lower, far_upper, far_lower):
    div = None
    for a in range(3):
        term = masked(upper[a], p[a]) - masked(far_lower[a], prev_p[a])
        div = term if div is None else div + term
    new_u = (u + primal_step * div) * b_map + a_map
    new_v = []
    for a in range(3):
        total = p[a]
        for b in range(3):
            here = masked(lower[b], q[ROWS_OF_Q[b][a]])
            total = total + (masked(far_upper[b], next_q[b][a]) - here)
        new_v.append(v[a] + primal_step * total)
    bar = [(2.0 * dual_step) * new_u - dual_step * u]
    bar += [(2.0 * dual_step) * new_v[a] - dual_step * v[a] for a in range(3)]
    return new_u, new_v, bar


DEPTH = 2


def pipelined(*passes):
    waiting = []
    for store in itertools.chain(*passes):
        waiting.append(store)
        if len(waiting) > DEPTH:
            waiting.pop(0)()
    for store in waiting:
        store()


class Steps:
    def __init__(self, extents, sizes, pos, ext, bars, side, side_bars):
        self.nz, self.ny, self.nx = nz, ny, nx = extents
        self.levels = nz + 2 * HALO
        self.pos, self.ext, self.bars, self.side, self.side_bars = pos, ext, bars, side, side_bars
        self.starts = tile_starts(ny)
        self.lane, slot = lanes_of()
        sub = lax.broadcasted_iota(jnp.int32, (8, LANES), 0)
        self.full = full = [sizes[axis] * extent for axis, extent in zip(AXES, (nx, ny, nz))]

        def masks(places, extent):
            upper = jnp.logical_and(places >= 0, places < extent - 1)
            lower = jnp.logical_and(places > 0, places < extent)
            return upper.astype(jnp.float32), lower.astype(jnp.float32)

        def tiles(rows):
            outer = (rows[0], rows[-1])
            return [
                (row,) + (masks(pos[1] * ny + (row - ROW0) + sub, full[1]) if row in outer else (None, None))
                for row in rows
            ]

        self.tiles = tiles(self.starts)
        self.own_tiles = tiles(list(range(ROW0, ROW0 + ny, 8)))
        self.x_main = masks(pos[0] * nx + self.lane, full[0])
        self.x_side = [masks(pos[0] * nx + at + slot, full[0]) for at in (-HALO, nx - HALO)]
        self.z_side = masks(pos[2] * nz - HALO + self.lane // SLOT, full[2])
        self.first, self.last = self.lane == 0, self.lane == LANES - 1
        at_first, at_last = pos[0] == 0, pos[0] == sizes["gx"] - 1
        self.beyond = (
            jnp.logical_and(slot == HALO - 1, at_first),
            jnp.logical_and(slot == HALO, at_last),
        )

    def z_main(self, level):
        place = self.pos[2] * self.nz - HALO + level
        upper = jnp.logical_and(place >= 0, place < self.full[2] - 1)
        lower = jnp.logical_and(place > 0, place < self.full[2])
        one, none = jnp.float32(1.0), jnp.float32(0.0)
        upper, lower = jnp.where(upper, one, none), jnp.where(lower, one, none)
        return (upper if level == HALO + self.nz - 1 else None), (lower if level == HALO else None)

    def from_low(self, values, level):
        return pltpu.roll(values, LANES - HALO + 1 - SLOT * level, 1)

    def from_high(self, values, level):
        return pltpu.roll(values, LANES - 1 - HALO - SLOT * level, 1)

    def next_x(self, values, field_values, level):
        return jnp.where(self.last, self.from_high(field_values, level), pltpu.roll(values, LANES - 1, 1))

    def prev_x(self, values, field_values, level):
        return jnp.where(self.first, self.from_low(field_values, level), pltpu.roll(values, 1, 1))

    @staticmethod
    def maps(f, w):
        inverse = 1.0 / (1.0 + primal_step * w)
        return (primal_step * w * f) * inverse, inverse

    def prepare_main(self, level):
        for row in self.starts:
            here = pl.ds(row, 8)
            maps = self.maps(self.ext[F, level, here, :], self.ext[W, level, here, :])
            bar = [dual_step * self.ext[U + a, level, here, :] for a in range(4)]

            def store(here=here, maps=maps, bar=bar):
                self.ext[F, level, here, :], self.ext[W, level, here, :] = maps
                for a in range(4):
                    self.bars[a, level + 1, here, :] = bar[a]

            yield store

    def prepare_side(self, which, row, fields):
        here = pl.ds(row, 8)
        values = list(self.maps(fields[F], fields[W])) + fields[U:]
        bar = [dual_step * fields[U + a] for a in range(4)]

        def store():
            for field in range(FIELDS):
                self.side[field, which, here, :] = values[field]
            for a in range(4):
                self.side_bars[a, which, here, :] = bar[a]

        return store

    def p_main(self, level):
        ext, bars = self.ext, self.bars
        upper_z, _ = self.z_main(level)
        for row, upper_y, _ in self.tiles:
            here = pl.ds(row, 8)
            bar = [bars[a, level + 1, here, :] for a in range(4)]
            next_bar = [
                self.next_x(bar[0], self.side_bars[0, 1, here, :], level),
                bars[0, level + 1, pl.ds(row + 1, 8), :],
                bars[0, level + 2, here, :],
            ]
            p = [ext[PF + a, level, here, :] for a in range(3)]
            p = p_step(bar, next_bar, p, (self.x_main[0], upper_y, upper_z))

            def store(here=here, p=p):
                for a in range(3):
                    ext[PF + a, level, here, :] = p[a]

            yield store

    def q_main(self, level):
        ext, bars = self.ext, self.bars
        _, lower_z = self.z_main(level)
        for row, _, lower_y in self.tiles:
            here = pl.ds(row, 8)
            bar = [bars[1 + a, level + 1, here, :] for a in range(3)]
            prev_bar = [
                [self.prev_x(bar[a], self.side_bars[1 + a, 0, here, :], level) for a in range(3)],
                [bars[1 + a, level + 1, pl.ds(row - 1, 8), :] for a in range(3)],
                [bars[1 + a, level, here, :] for a in range(3)],
            ]
            q = [ext[QF + a, level, here, :] for a in range(6)]
            q = q_step(bar, prev_bar, q, (self.x_main[1], lower_y, lower_z))

            def store(here=here, q=q):
                for a in range(6):
                    ext[QF + a, level, here, :] = q[a]

            yield store

    def primal_main(self, level, final=False):
        ext, bars, side = self.ext, self.bars, self.side
        upper_z, lower_z = self.z_main(level)
        for row, upper_y, lower_y in self.own_tiles if final else self.tiles:
            here = pl.ds(row, 8)
            p = [ext[PF + a, level, here, :] for a in range(3)]
            q = [ext[QF + a, level, here, :] for a in range(6)]
            prev_p = [
                self.prev_x(p[0], side[PF, 0, here, :], level),
                ext[PF + 1, level, pl.ds(row - 1, 8), :],
                ext[PF + 2, level - 1, here, :],
            ]
            next_q = [
                [self.next_x(q[j], side[QF + j, 1, here, :], level) for j in ROWS_OF_Q[0]],
                [ext[QF + j, level, pl.ds(row + 1, 8), :] for j in ROWS_OF_Q[1]],
                [ext[QF + j, level + 1, here, :] for j in ROWS_OF_Q[2]],
            ]
            new_u, new_v, bar = primal_step_of(
                ext[U, level, here, :],
                [ext[V + a, level, here, :] for a in range(3)],
                ext[F, level, here, :],
                ext[W, level, here, :],
                p,
                q,
                prev_p,
                next_q,
                (self.x_main[0], upper_y, upper_z),
                (self.x_main[1], lower_y, lower_z),
                (None, upper_y, upper_z),
                (None, lower_y, lower_z),
            )

            def store(here=here, values=[new_u] + new_v, bar=bar):
                for a in range(4):
                    ext[U + a, level, here, :] = values[a]
                for a in () if final else range(4):
                    bars[a, level + 1, here, :] = bar[a]

            yield store

    def dual_side(self, z_masks, final=False):
        side, side_bars = self.side, self.side_bars
        z_upper, z_lower = z_masks
        for which, (row, upper_y, lower_y) in itertools.product((0, 1), self.tiles):
            here = pl.ds(row, 8)
            bar = [side_bars[a, which, here, :] for a in range(4)]
            if not (final and which == 1):
                next_bar = [
                    pltpu.roll(bar[0], LANES - 1, 1),
                    side_bars[0, which, pl.ds(row + 1, 8), :],
                    pltpu.roll(bar[0], LANES - SLOT, 1),
                ]
                upper = (self.x_side[which][0], upper_y, z_upper)
                p = p_step(bar, next_bar, [side[PF + a, which, here, :] for a in range(3)], upper)
                if which == 0:
                    p[0] = jnp.where(self.beyond[0], 0.0, p[0])

                def store(which=which, here=here, p=p):
                    for a in range(3):
                        side[PF + a, which, here, :] = p[a]

                yield store
            if not (final and which == 0):
                prev_bar = [
                    [pltpu.roll(bar[1 + a], 1, 1) for a in range(3)],
                    [side_bars[1 + a, which, pl.ds(row - 1, 8), :] for a in range(3)],
                    [pltpu.roll(bar[1 + a], SLOT, 1) for a in range(3)],
                ]
                lower = (self.x_side[which][1], lower_y, z_lower)
                q = q_step(bar[1:], prev_bar, [side[QF + a, which, here, :] for a in range(6)], lower)
                if which == 1:
                    for a in ROWS_OF_Q[0]:
                        q[a] = jnp.where(self.beyond[1], 0.0, q[a])

                def store(which=which, here=here, q=q):
                    for a in range(6):
                        side[QF + a, which, here, :] = q[a]

                yield store

    def primal_side(self, z_masks):
        side, side_bars = self.side, self.side_bars
        for which, (row, upper_y, lower_y) in itertools.product((0, 1), self.tiles):
            here = pl.ds(row, 8)
            p = [side[PF + a, which, here, :] for a in range(3)]
            q = [side[QF + a, which, here, :] for a in range(6)]
            prev_p = [
                pltpu.roll(p[0], 1, 1),
                side[PF + 1, which, pl.ds(row - 1, 8), :],
                pltpu.roll(p[2], SLOT, 1),
            ]
            next_q = [
                [pltpu.roll(q[j], LANES - 1, 1) for j in ROWS_OF_Q[0]],
                [side[QF + j, which, pl.ds(row + 1, 8), :] for j in ROWS_OF_Q[1]],
                [pltpu.roll(q[j], LANES - SLOT, 1) for j in ROWS_OF_Q[2]],
            ]
            upper = (self.x_side[which][0], upper_y, z_masks[0])
            lower = (self.x_side[which][1], lower_y, z_masks[1])
            new_u, new_v, bar = primal_step_of(
                side[U, which, here, :],
                [side[V + a, which, here, :] for a in range(3)],
                side[F, which, here, :],
                side[W, which, here, :],
                p,
                q,
                prev_p,
                next_q,
                upper,
                lower,
                upper,
                lower,
            )

            def store(which=which, here=here, values=[new_u] + new_v, bar=bar):
                for a in range(4):
                    side[U + a, which, here, :] = values[a]
                    side_bars[a, which, here, :] = bar[a]

            yield store


def solve_inner(extents, sizes, ext_in, side_in, ext, bars, side, side_bars):
    pos = place_of()
    del ext_in
    nz, _, _ = extents
    steps = Steps(extents, sizes, pos, ext, bars, side, side_bars)

    def strips():
        for which, row in itertools.product((0, 1), steps.starts):
            fields = [side_in[field, which, pl.ds(row, 8), :] for field in range(FIELDS)]
            yield steps.prepare_side(which, row, fields)

    pipelined(strips(), *(steps.prepare_main(level) for level in range(HALO, HALO + nz)))
    inside = (None, None)
    for step in range(ITERS):
        final = step == ITERS - 1
        low, high = HALO + step, HALO + nz - step
        pipelined(
            steps.dual_side(inside, final),
            *(steps.p_main(level) for level in range(low, high - 1)),
            *(steps.q_main(level) for level in range(low + 1, high)),
        )
        pipelined(
            *(() if final else (steps.primal_side(inside),)),
            *(steps.primal_main(level, final) for level in range(low + 1, high - 1)),
        )


def solve_outer(extents, sizes, ys, zs, ext_in, bars_in, side_in, *rest):
    pos = place_of()
    del ext_in, bars_in
    nz, ny, _ = extents
    z_got = dict(zip(zs, rest))
    rest = rest[len(zs) :]
    frame_got = dict(zip(zs, rest))
    ext, bars, out_u, out_v, out_p, out_q, side, side_bars, sem = rest[len(zs) :]
    steps = Steps(extents, sizes, pos, ext, bars, side, side_bars)
    starts = steps.starts
    lane, slot = lanes_of()
    sides = ("low", "high")

    for z_parity in (0, 1):

        @pl.when(pos[2] % 2 == z_parity)
        def _():
            for z_side in sides:
                got = pick(z_got, colour_of(z_side, z_parity))
                for i, (field, at) in enumerate(placed(z_side, nz)):
                    ext[field, HALO + at, pl.ds(ROW0, ny), :] = got[i]

    for z_parity, y_parity in itertools.product((0, 1), (0, 1)):

        @pl.when(jnp.logical_and(pos[2] % 2 == z_parity, pos[1] % 2 == y_parity))
        def _():
            for z_side, y_side in itertools.product(sides, sides):
                got = pick(frame_got, colour_of(z_side, z_parity))
                y_colour = colour_of(y_side, y_parity)
                n = ys.index(y_colour) if y_colour in ys else 0
                first = BLOCKS * 8 * len(starts) + n * SENT * HALO
                row = ROW0 + (-HALO if y_side == "low" else ny)
                for i, (field, at) in enumerate(placed(z_side, nz)):
                    ext[field, HALO + at, pl.ds(row, HALO), :] = got[pl.ds(first + i * HALO, HALO), :]

    top = (HALO + nz) * SLOT
    below, above = lane < BLOCK, lane >= top
    low_levels, high_levels = range(HALO), range(HALO + nz, nz + 2 * HALO)

    outer = jnp.logical_or(below, above)

    def strips(got_low, got_high):
        for j, row in enumerate(starts):
            here = pl.ds(row, 8)
            fields = ([], [])
            for field in range(FIELDS):
                block, k = divmod(field, PER_TILE)
                columns = None
                for level in list(low_levels) + list(high_levels):
                    turned = columns_of(ext[field, level, here, :], level)
                    columns = turned if columns is None else jnp.where(lane >= level * SLOT, turned, columns)
                at = (pl.ds(8 * (block * len(starts) + j), 8), slice(None))
                came = jnp.where(
                    above,
                    pltpu.roll(got_high[at], (top - k * BLOCK) % LANES, 1),
                    pltpu.roll(got_low[at], (-k * BLOCK) % LANES, 1),
                )
                left = jnp.where(slot < HALO, came, columns)
                right = jnp.where(slot < HALO, columns, came)
                fields[0].append(jnp.where(outer, left, side_in[field, 0, here, :]))
                fields[1].append(jnp.where(outer, right, side_in[field, 1, here, :]))
            made = [steps.prepare_side(which, row, fields[which]) for which in (0, 1)]
            yield from made

    for z_parity in (0, 1):

        @pl.when(pos[2] % 2 == z_parity)
        def _():
            low, high = (pick(frame_got, colour_of(z_side, z_parity)) for z_side in sides)
            pipelined(strips(low, high))

    pipelined(*(steps.prepare_main(level) for level in list(low_levels) + list(high_levels)))

    def out_copies(fields):
        own = (pl.ds(HALO, nz), pl.ds(ROW0, ny))
        return [pltpu.make_async_copy(ext.at[(field,) + own], out, sem) for field, out in fields]

    duals = [(pl.ds(PF, 3), out_p), (pl.ds(QF, 6), out_q)]
    primals = [(U, out_u), (pl.ds(V, 3), out_v)]

    def outer_levels(low_first, high_first):
        return sorted({first + j for first in (low_first, high_first) for j in range(HALO)})

    for step in range(ITERS):
        final = step == ITERS - 1
        top_level = HALO + nz - 1 - step
        pipelined(
            steps.dual_side(steps.z_side, final),
            *(steps.p_main(level) for level in outer_levels(step, top_level)),
            *(steps.q_main(level) for level in outer_levels(step + 1, top_level + 1)),
        )
        if final:
            for copy in out_copies(duals):
                copy.start()
        pipelined(
            *(() if final else (steps.primal_side(steps.z_side),)),
            *(steps.primal_main(level, final) for level in outer_levels(step + 1, top_level)),
        )
    for copy in out_copies(primals):
        copy.start()
    for copy in out_copies(duals + primals):
        copy.wait()


def per_device(sizes, noisy_image, fidelity, primal_u, primal_v, dual_p, dual_q):
    nz, ny, nx = extents = noisy_image.shape
    levels, rows = nz + 2 * HALO, ny + 2 * ROW0
    assert nx == LANES and ny % 8 == 0 and nz * SLOT <= LANES // 2
    assert min(nz, ny) >= HALO and min(sizes.values()) > 1
    xs, ys, zs = (colours(sizes[axis]) for axis in AXES)
    args = tuple(pltpu.with_memory_space_constraint(a, pltpu.HBM) for a in (noisy_image, fidelity, primal_u, primal_v, dual_p, dual_q))
    f32 = jnp.float32
    anywhere = pl.BlockSpec(memory_space=pltpu.HBM)
    vmem = pl.BlockSpec(memory_space=pltpu.VMEM)

    def shaped(*shape):
        return jax.ShapeDtypeStruct(shape, f32)

    def call(body, ins, outs, out_specs, limit, **more):
        return pl.pallas_call(
            body,
            in_specs=ins,
            out_specs=out_specs,
            out_shape=outs,
            compiler_params=pltpu.CompilerParams(vmem_limit_bytes=limit * 1024 * 1024),
            **more,
        )

    strip_rows = 8 * len(tile_starts(ny))
    ext_shape = shaped(FIELDS, levels, rows, nx)
    packed = call(
        functools.partial(pack, extents, ys, zs),
        [anywhere] * 6,
        [ext_shape] + [shaped(SENT, nz, nx)] * len(ys) + [shaped(SENT, ny, nx)] * len(zs),
        [vmem] * (1 + len(ys) + len(zs)),
        16,
        scratch_shapes=[pltpu.SemaphoreType.DMA, pltpu.SemaphoreType.DMA],
    )(*args)
    ext, y_pay, z_pay = packed[0], packed[1 : 1 + len(ys)], packed[1 + len(ys) :]
    y_got = [exchange(pay, {"gy": c}, sizes) for c, pay in zip(ys, y_pay)]
    z_got = [exchange(pay, {"gz": c}, sizes) for c, pay in zip(zs, z_pay)]

    ext, x_pay = call(
        functools.partial(join_y, extents, ys),
        [vmem] * (1 + len(ys)),
        [ext_shape, shaped(GROUPS, strip_rows, nx)],
        [vmem] * 2,
        16,
        input_output_aliases={0: 0},
    )(ext, *y_got)
    x_got = [exchange(x_pay, {"gx": c}, sizes) for c in xs]

    both = shaped(FIELDS, 2, rows, nx)
    frame = shaped(BLOCKS * strip_rows + len(ys) * SENT * HALO, nx)
    side, *frame_pay = call(
        functools.partial(join_x, extents, xs, ys, zs),
        [vmem] * (2 + len(xs)),
        [shaped(2 * GROUPS, 2, rows, nx)] + [frame] * len(zs),
        [vmem] * (1 + len(zs)),
        16,
    )(ext, x_pay, *x_got)
    frame_got = [exchange(pay, {"gz": c}, sizes) for c, pay in zip(zs, frame_pay)]

    bar_shape = shaped(4, levels + 2, rows, nx)
    scratch = [pltpu.VMEM(both.shape, f32), pltpu.VMEM((4,) + both.shape[1:], f32)]
    ext, bars = call(
        functools.partial(solve_inner, extents, sizes),
        [vmem] * 2,
        [ext_shape, bar_shape],
        [vmem] * 2,
        16,
        input_output_aliases={0: 0},
        scratch_shapes=scratch,
    )(ext, side)

    solved = call(
        functools.partial(solve_outer, extents, sizes, ys, zs),
        [vmem] * (3 + 2 * len(zs)),
        [ext_shape, bar_shape] + [shaped(*a.shape) for a in (primal_u, primal_v, dual_p, dual_q)],
        [vmem] * 2 + [anywhere] * 4,
        24,
        input_output_aliases={0: 0, 1: 1},
        scratch_shapes=scratch + [pltpu.SemaphoreType.DMA],
    )(ext, bars, side, *z_got, *frame_got)
    return tuple(solved[2:])


def solution(mesh):
    sizes = {axis: mesh.shape[axis] for axis in AXES}
    scalar, stacked = P("gz", "gy", "gx"), P(None, "gz", "gy", "gx")

    def body(*args):
        return per_device(sizes, *args)

    return jax.shard_map(
        body,
        mesh=mesh,
        in_specs=(scalar,) * 3 + (stacked,) * 3,
        out_specs=(scalar,) + (stacked,) * 3,
        check_vma=False,
    )
```
